128 devices in a mesh: dp: 8 (over y_lo, x), tensor: 16 (over y_hi, z, core).
Axes of the slice: x: 4, y: 4 (y_hi: 2, y_lo: 2; y = y_hi * 2 + y_lo), z: 4, core: 2. Of those that a mesh axis runs over, the one named last changes fastest.
Arguments:
- tokens: bfloat16 [8192, 4096], P(('dp', 'tensor')), parts along dimension 0, may hold values from -6 to 6
- norm_gain: float32 [4096], replicated, may hold values from 0.5 to 1.5
- gate_weight: bfloat16 [4096, 14336], P(None, 'tensor'), may hold values from -0.09375 to 0.09375
- up_weight: bfloat16 [4096, 14336], P(None, 'tensor'), may hold values from -0.09375 to 0.09375
- down_weight: bfloat16 [14336, 4096], P('tensor'), may hold values from -0.0625 to 0.0625
Outputs:
- mixed: bfloat16 [8192, 4096], P('dp', 'tensor'), parts along dimension 0
The draws below stay inside these ranges and needn't reach their ends.
There are 8 independent parts, one for each index of `dp`. The reference program is written for one: setup_inputs(seed, part) draws one part's arguments, and reference() takes and returns one part's arrays. A program takes and returns all parts, laid end to end along the dimension named above; an argument that names none is the same for every part. Nothing has to cross between parts.
All inputs are finite; a program needn't handle non-finite values.
Results may differ from the reference program's by a relative error of at most 0.0053.
Values may be sent and summed in bfloat16 or wider, within the bound.
A program may use at most 128 MiB of HBM per device.

```python
import jax
import jax.numpy as jnp
from jax import lax

D = 4096
FF = 14336
TOKENS = 1024


def raised(entries, key, source, target, blocks, factor):
    owner, partner = [(jnp.arange(entries.shape[axis_at]) // (entries.shape[axis_at] // blocks)).reshape([-1 if axis == axis_at else 1 for axis in range(entries.ndim)]) for axis_at in (source, target)]
    chosen = jax.random.permutation(key, blocks)[partner]
    strong = (owner == chosen) | (owner == (partner + blocks // 2) % blocks)
    return jnp.where(strong, factor * entries, entries)


def levels(rng, extent, cuts, smallest, high):
    factor_of = 1.0
    for axis_at, parts in cuts:
        heights = jax.random.uniform(jax.random.fold_in(jax.random.fold_in(rng, 6), axis_at), (parts,), jnp.float32, smallest / len(cuts), high / len(cuts))
        factor_of = factor_of * jnp.repeat(jnp.exp(heights), extent[axis_at] // parts).reshape((-1,) + (1,) * (len(extent) - 1 - axis_at))
    return factor_of


def centred(stream_key, dims, spread, most, cuts=(), dtype=jnp.bfloat16):
    gain = levels(stream_key, dims, cuts, -0.22, 0.18) if cuts else 1.0
    drawn = jax.random.normal(stream_key, dims, jnp.float32) * spread * gain
    return jnp.minimum(jnp.maximum(drawn, -most), most).astype(dtype)


def bell_draw_with(rng, extent, spread, bound, shards, heavy, held_as=jnp.bfloat16):
    entries = spread * jax.random.normal(rng, extent, jnp.float32)
    if shards:
        entries = entries * levels(rng, extent, shards, -0.22, 0.18)
    return jnp.clip(raised(entries, jax.random.fold_in(rng, 3), *heavy), -bound, bound).astype(held_as)


def setup_inputs(seed: int = 0, part: int = 0) -> dict:
    streams_of = jax.random.split(jax.random.key(seed), 6)
    part_keys = jax.random.split(jax.random.fold_in(streams_of[5], part), 6)
    tokens = centred(part_keys[0], (TOKENS, D), 1.0, 6.0, ((0, 16),))
    norm_gain = jnp.clip(1.0 + 0.1 * jax.random.normal(streams_of[1], (D,), jnp.float32), 0.5, 1.5)
    gate_weight = centred(streams_of[2], (D, FF), D ** -0.5, 0.09375, ((1, 16),))
    up_weight = centred(streams_of[3], (D, FF), D ** -0.5, 0.09375, ((1, 16),))
    down_weight = bell_draw_with(streams_of[4], (FF, D), FF ** -0.5, 0.0625, ((0, 16),), (0, 1, 16, 2.0))
    return {"tokens": tokens, "norm_gain": norm_gain, "gate_weight": gate_weight, "up_weight": up_weight, "down_weight": down_weight}


def reference(tokens, norm_gain, gate_weight, up_weight, down_weight):
    wide = tokens.astype(jnp.float32)
    square_mean = lax.optimization_barrier(jnp.mean(wide * wide, axis=1, keepdims=True))
    normed = (wide * norm_gain[None, :] / jnp.sqrt(square_mean + 1e-05)).astype(jnp.bfloat16)
    gate = jnp.dot(normed, gate_weight, preferred_element_type=jnp.float32)
    up = jnp.dot(normed, up_weight, preferred_element_type=jnp.float32)
    hidden = (jax.nn.silu(gate) * up).astype(jnp.bfloat16)
    branch = jnp.dot(hidden, down_weight, preferred_element_type=jnp.float32)
    return (wide + branch).astype(jnp.bfloat16)
```

```python
import jax
import jax.numpy as jnp
from jax import lax
from jax.experimental import pallas as pl
from jax.experimental.pallas import tpu as pltpu
from jax.sharding import PartitionSpec as P

MESH = pl.DeviceIdType.MESH
F32, BF16 = jnp.float32, jnp.bfloat16
D, F, ROWS, COLS = 4096, 896, 1024, 256

SLOTS = [(0, 0), (0, 1), (0, 3), (1, 0), (0, 2), (1, 1), (1, 3), (1, 2)]
DESTS = [(1, 2), (1, 1), (1, 3), (0, 2), (1, 0), (0, 1), (0, 3), (0, 0)]
SLOT = {b: i for i, b in enumerate(SLOTS)}
DEST = {b: i for i, b in enumerate(DESTS)}
CHUNKS = {"A": (0, 1), "B": (1, 2), "C": (3, 2), "D": (5, 2), "E": (7, 1)}
PIECES = [(0, 3), (3, 2), (5, 3)]
SEEN = {
    "zp": lambda q, k: (q, (k + 1) % 4),
    "zm": lambda q, k: (q, (k + 3) % 4),
    "y": lambda q, k: (1 - q, k),
}


def kernel(tok_hbm, gain_ref, gate_hbm, up_hbm, down_hbm, out_hbm,
           x, w, dn, res, hid, own, sb, rb, sd, yl, zl, zh, yf, zf, out,
           local_sem, out_sem, bar_unused, ss, rs):
    dp, t = lax.axis_index("dp"), lax.axis_index("tensor")
    hi, z, c = t // 8, lax.rem(t // 2, 4), lax.rem(t, 2)

    def member(q, k, core):
        return (hi if q == 0 else 1 - hi) * 8 + lax.rem(z + k, 4) * 2 + core

    peer = {
        "zp": (dp, member(0, 1, c)),
        "zm": (dp, member(0, 3, c)),
        "y": (dp, member(1, 0, c)),
        "s": (dp, member(0, 0, 1 - c)),
    }

    mine = pl.ds(pl.multiple_of(c * 64, 64), 64)
    other = pl.ds(pl.multiple_of((1 - c) * 64, 64), 64)
    tok_copy = pltpu.make_async_copy(tok_hbm, res.at[mine], local_sem.at[0])
    tok_copy.start()
    w_copies, d_copies = [], []
    for j in range(7):
        for part, src in enumerate((gate_hbm, up_hbm)):
            w_copies.append(pltpu.make_async_copy(
                src.at[:, pl.ds(j * 128, 128)], w.at[:, pl.ds(j * 256 + part * 128, 128)],
                local_sem.at[1 + 2 * j + part]))
    for r, (q, k) in enumerate(DESTS):
        for part, core in enumerate((1 - c, c)):
            col = pl.multiple_of(member(q, k, core) * COLS, COLS)
            d_copies.append(pltpu.make_async_copy(
                down_hbm.at[:, pl.ds(col, COLS)], dn.at[:, pl.ds((2 * r + part) * COLS, COLS)],
                local_sem.at[15 + 2 * r + part]))
    for copy in w_copies + d_copies:
        copy.start()

    barrier = pltpu.get_barrier_semaphore()
    for link in ("zp", "zm", "y", "s"):
        pl.semaphore_signal(barrier, inc=1, device_id=peer[link], device_id_type=MESH)

    count = [0]

    def remote(link, src, dst):
        i = count[0]
        count[0] += 1
        return pltpu.make_async_remote_copy(
            src_ref=src, dst_ref=dst, send_sem=ss.at[i], recv_sem=rs.at[i],
            device_id=peer[link], device_id_type=MESH)

    started = []

    def start(copy):
        copy.start()
        started.append(copy)

    def rows_of(block, h):
        return pl.ds(pl.multiple_of(SLOT[block] * 128 + c * 64 + h * 32, 32), 32)

    def gather(link, src, dst, h):
        return remote(link, x.at[rows_of(src, h)], x.at[rows_of(dst, h)])

    zp0 = [gather("zp", (0, 0), (0, 3), h) for h in range(2)]
    zm0 = [gather("zm", (0, 0), (0, 1), h) for h in range(2)]
    y0 = [gather("y", (0, 0), (1, 0), h) for h in range(2)]
    zp2 = gather("zp", (0, 3), (0, 2), 0)
    zm2 = gather("zm", (0, 1), (0, 2), 1)
    zpp = [gather("zp", (1, 0), (1, 3), h) for h in range(2)]
    zmp = [gather("zm", (1, 0), (1, 1), h) for h in range(2)]
    y2 = [gather("y", (0, 2), (1, 2), h) for h in range(2)]
    sib = {b: [gather("s", b, b, h) for h in range(2)] for b in SLOTS}

    def pair(chunk, first, last):
        lo, n = CHUNKS[chunk]
        part = (pl.ds(first, last - first), pl.ds(lo * 128, n * 128))
        return remote("s", sb.at[part], rb.at[part])

    pairs = {}
    for name in CHUNKS:
        pairs[name] = [pair(name, 0, 3), pair(name, 3, 8)]
    leaf = {}
    for name, (lo, n) in CHUNKS.items():
        part = pl.ds(lo * 128, n * 128)
        leaf[name] = {
            "y": remote("y", sd.at[DEST[1, 2], part], yl.at[part]),
            "zp": remote("zp", sd.at[DEST[1, 1], part], zl.at[0, part]),
            "zm": remote("zm", sd.at[DEST[1, 3], part], zl.at[1, part]),
        }
    half, across, last = [], [], []
    for lo, n in PIECES:
        part = pl.ds(lo * 128, n * 128)
        half.append({
            "zp": remote("zp", sd.at[DEST[0, 2], part, pl.ds(0, 128)], zh.at[0, part]),
            "zm": remote("zm", sd.at[DEST[0, 2], part, pl.ds(128, 128)], zh.at[1, part]),
        })
        across.append(remote("y", sd.at[DEST[1, 0], part], yf.at[part]))
        last.append({
            "zp": remote("zp", sd.at[DEST[0, 1], part], zf.at[0, part]),
            "zm": remote("zm", sd.at[DEST[0, 3], part], zf.at[1, part]),
        })

    waited = set()

    def arrived(copy):
        if id(copy) not in waited:
            waited.add(id(copy))
            copy.wait_recv()

    def leaf_with(link, slot):
        s = SLOT[SEEN[link](*SLOTS[slot])]
        for name, (lo, n) in CHUNKS.items():
            if lo <= s < lo + n:
                arrived(leaf[name][link])
        return pl.ds(s * 128, 128)

    def piece_with(link, messages, slot):
        s = SLOT[SEEN[link](*SLOTS[slot])]
        for i, (lo, n) in enumerate(PIECES):
            if lo <= s < lo + n:
                arrived(messages[i] if link == "y" else messages[i][link])
        return pl.ds(s * 128, 128)

    res[other] = jnp.zeros((64, D), BF16)
    tok_copy.wait()
    gain = gain_ref[...]
    for i in range(4):
        wide = res[pl.ds(pl.multiple_of(c * 64 + i * 16, 16), 16)].astype(F32)
        square_mean = jnp.mean(wide * wide, axis=1, keepdims=True)
        normed = wide * gain / jnp.sqrt(square_mean + 1e-05)
        x[pl.ds(pl.multiple_of(c * 64 + i * 16, 16), 16)] = normed.astype(BF16)
    pl.semaphore_wait(barrier, 4)

    for copy in (zp0[0], zm0[1], y0[0], sib[0, 0][0], sib[0, 0][1], zp0[1], zm0[0], y0[1]):
        start(copy)

    def dot_in(name):
        lo, n = CHUNKS[name]
        rows = pl.ds(lo * 128, n * 128)
        both = jnp.dot(x[rows], w[...], preferred_element_type=F32)
        for j in range(7):
            gate, up = both[:, j * 256:j * 256 + 128], both[:, j * 256 + 128:j * 256 + 256]
            hid[rows, pl.ds(j * 128, 128)] = (gate / (1.0 + jnp.exp(-gate)) * up).astype(BF16)

    def dot_out(name, first, last):
        lo, n = CHUNKS[name]
        rows = pl.ds(lo * 128, n * 128)
        part = jnp.dot(hid[rows], dn[:, pl.ds(first * 512, (last - first) * 512)], preferred_element_type=F32)
        for r in range(first, last):
            for side in range(2):
                at = (r - first) * 512 + side * 256
                value = part[:, at:at + 256]
                if name == "A":
                    core = (1 - c, c)[side]
                    col = pl.multiple_of(member(*DESTS[r], core) * COLS, COLS)
                    value = value + res[:, pl.ds(col, COLS)].astype(F32)
                if side == 0:
                    sb[r, rows] = value.astype(BF16)
                else:
                    own[r, rows] = value

    def chip_sum(r, slot):
        rows = pl.ds(slot * 128, 128)
        return own[r, rows] + rb[r, rows].astype(F32)

    def send_leaf(name):
        lo, n = CHUNKS[name]
        arrived(pairs[name][0])
        for link, dest in (("y", (1, 2)), ("zp", (1, 1)), ("zm", (1, 3))):
            r = DEST[dest]
            for slot in range(lo, lo + n):
                sd[r, pl.ds(slot * 128, 128)] = chip_sum(r, slot).astype(BF16)
            start(leaf[name][link])

    def pair_rest(lo, n):
        for name, (a, m) in CHUNKS.items():
            if a < lo + n and lo < a + m:
                arrived(pairs[name][1])

    def send_half(i):
        lo, n = PIECES[i]
        pair_rest(lo, n)
        r = DEST[0, 2]
        for slot in range(lo, lo + n):
            got = leaf_with("y", slot)
            sd[r, pl.ds(slot * 128, 128)] = (chip_sum(r, slot) + yl[got].astype(F32)).astype(BF16)
        start(half[i]["zp"])
        start(half[i]["zm"])

    def send_across(i):
        lo, n = PIECES[i]
        pair_rest(lo, n)
        r = DEST[1, 0]
        for slot in range(lo, lo + n):
            value = chip_sum(r, slot)
            value = value + zl[0, leaf_with("zp", slot)].astype(F32)
            value = value + zl[1, leaf_with("zm", slot)].astype(F32)
            sd[r, pl.ds(slot * 128, 128)] = value.astype(BF16)
        start(across[i])

    def send_last(i):
        lo, n = PIECES[i]
        for link, dest, side in (("zp", (0, 1), 0), ("zm", (0, 3), 1)):
            r = DEST[dest]
            for slot in range(lo, lo + n):
                rows = pl.ds(slot * 128, 128)
                value = chip_sum(r, slot)
                got = zh[side, piece_with(link, half, slot)].astype(F32)
                keep = (1 - side) * 128
                sd[r, rows, pl.ds(side * 128, 128)] = (value[:, side * 128:side * 128 + 128] + got).astype(BF16)
                sd[r, rows, pl.ds(keep, 128)] = value[:, keep:keep + 128].astype(BF16)
            start(last[i][link])

    out_copies = []

    def finish(slot):
        q, k = SLOTS[slot]
        rows = pl.ds(slot * 128, 128)
        value = chip_sum(DEST[0, 0], slot)
        value = value + yf[piece_with("y", across, slot)].astype(F32)
        value = value + zf[0, piece_with("zp", last, slot)].astype(F32)
        value = value + zf[1, piece_with("zm", last, slot)].astype(F32)
        out[rows] = value.astype(BF16)
        at = pl.multiple_of(member(q, k, 0) * 64, 128)
        copy = pltpu.make_async_copy(out.at[rows], out_hbm.at[pl.ds(at, 128)], out_sem.at[slot])
        copy.start()
        out_copies.append(copy)

    def both_halves(block):
        arrived(sib[block][0])
        arrived(sib[block][1])

    both_halves((0, 0))
    for copy in w_copies:
        copy.wait()
    dot_in("A")
    arrived(zp0[0])
    start(zp2)
    start(sib[0, 3][0])
    arrived(zm0[1])
    start(zm2)
    start(sib[0, 1][1])
    arrived(y0[0])
    start(zpp[0])
    start(zmp[0])
    start(sib[1, 0][0])
    for copy in d_copies:
        copy.wait()
    dot_out("A", 0, 3)
    start(pairs["A"][0])
    dot_out("A", 3, 8)
    start(pairs["A"][1])
    arrived(zp0[1])
    start(sib[0, 3][1])
    arrived(zm0[0])
    start(sib[0, 1][0])
    arrived(y0[1])
    start(zpp[1])
    start(zmp[1])
    start(sib[1, 0][1])
    send_leaf("A")
    both_halves((0, 1))
    both_halves((0, 3))
    dot_in("B")
    arrived(zp2)
    start(y2[0])
    start(sib[0, 2][0])
    arrived(zm2)
    start(y2[1])
    start(sib[0, 2][1])
    dot_out("B", 0, 3)
    start(pairs["B"][0])
    dot_out("B", 3, 8)
    start(pairs["B"][1])
    both_halves((1, 0))
    both_halves((0, 2))
    dot_in("C")
    send_leaf("B")
    arrived(zpp[0])
    start(sib[1, 3][0])
    arrived(zmp[0])
    start(sib[1, 1][0])
    dot_out("C", 0, 3)
    start(pairs["C"][0])
    dot_out("C", 3, 8)
    start(pairs["C"][1])
    send_leaf("C")
    arrived(zpp[1])
    start(sib[1, 3][1])
    arrived(zmp[1])
    start(sib[1, 1][1])
    both_halves((1, 1))
    both_halves((1, 3))
    dot_in("D")
    arrived(y2[0])
    start(sib[1, 2][0])
    arrived(y2[1])
    start(sib[1, 2][1])
    dot_out("D", 0, 3)
    start(pairs["D"][0])
    send_across(0)
    both_halves((1, 2))
    dot_in("E")
    send_leaf("D")
    dot_out("E", 0, 3)
    start(pairs["E"][0])
    dot_out("D", 3, 8)
    start(pairs["D"][1])
    send_leaf("E")
    dot_out("E", 3, 8)
    start(pairs["E"][1])
    send_half(0)
    send_half(1)
    send_across(1)
    send_half(2)
    send_across(2)
    send_last(0)
    send_last(1)
    send_last(2)
    for slot in range(8):
        finish(slot)
    for copy in started:
        copy.wait_send()
    for copy in out_copies:
        copy.wait()


N_REMOTE = 14 + 16 + 10 + 15 + 15
ANY, VMEM = pl.BlockSpec(memory_space=pl.ANY), pl.BlockSpec(memory_space=pltpu.VMEM)


def on_device(tokens, norm_gain, gate_weight, up_weight, down_weight):
    return pl.pallas_call(
        kernel,
        out_shape=jax.ShapeDtypeStruct((ROWS, COLS), BF16),
        in_specs=[ANY, VMEM, ANY, ANY, ANY],
        out_specs=ANY,
        scratch_shapes=[
            pltpu.VMEM((ROWS, D), BF16),
            pltpu.VMEM((D, 2 * F), BF16),
            pltpu.VMEM((F, D), BF16),
            pltpu.VMEM((128, D), BF16),
            pltpu.VMEM((ROWS, F), BF16),
            pltpu.VMEM((8, ROWS, COLS), F32),
            pltpu.VMEM((8, ROWS, COLS), BF16),
            pltpu.VMEM((8, ROWS, COLS), BF16),
            pltpu.VMEM((7, ROWS, COLS), BF16),
            pltpu.VMEM((ROWS, COLS), BF16),
            pltpu.VMEM((2, ROWS, COLS), BF16),
            pltpu.VMEM((2, ROWS, 128), BF16),
            pltpu.VMEM((ROWS, COLS), BF16),
            pltpu.VMEM((2, ROWS, COLS), BF16),
            pltpu.VMEM((ROWS, COLS), BF16),
            pltpu.SemaphoreType.DMA((31,)),
            pltpu.SemaphoreType.DMA((8,)),
            pltpu.SemaphoreType.REGULAR,
            pltpu.SemaphoreType.DMA((N_REMOTE,)),
            pltpu.SemaphoreType.DMA((N_REMOTE,)),
        ],
        compiler_params=pltpu.CompilerParams(
            collective_id=0, has_side_effects=True, vmem_limit_bytes=67043328),
    )(tokens, norm_gain.reshape(1, D), gate_weight, up_weight, down_weight)


def solution(mesh):
    return jax.shard_map(
        on_device,
        mesh=mesh,
        in_specs=(
            P(("dp", "tensor"), None),
            P(),
            P(None, "tensor"),
            P(None, "tensor"),
            P("tensor", None),
        ),
        out_specs=P("dp", "tensor"),
        check_vma=False,
    )
```

```python
import jax
import jax.numpy as jnp
from jax import lax
from jax.experimental import pallas as pl
from jax.experimental.pallas import tpu as pltpu
from jax.sharding import PartitionSpec as P

MESH = pl.DeviceIdType.MESH
F32, BF16 = jnp.float32, jnp.bfloat16
D, F, ROWS, COLS = 4096, 896, 1024, 256

UNITS = [(0, 0, 0), (0, 0, 1),
         (0, 3, 0), (0, 1, 1), (1, 0, 0),
         (1, 0, 1), (0, 2, 0), (0, 2, 1),
         (0, 3, 1), (0, 1, 0),
         (1, 3, 0), (1, 1, 0), (1, 2, 0), (1, 2, 1),
         (1, 3, 1), (1, 1, 1)]
UNIT = {b: i for i, b in enumerate(UNITS)}
CHUNKS = {"A": (0, 2), "B": (2, 3), "C": (5, 3), "D": (8, 2), "E": (10, 4), "F": (14, 2)}
PIECES = {"AB": (0, 5), "C": (5, 3), "D": (8, 2), "E": (10, 4), "F": (14, 2)}
DESTS = [(1, 2), (1, 1), (1, 3), (0, 2), (1, 0), (0, 1), (0, 3), (0, 0)]
DEST = {b: i for i, b in enumerate(DESTS)}
SEEN = {
    "zp": lambda q, k, h: (q, (k + 1) % 4, h),
    "zm": lambda q, k, h: (q, (k + 3) % 4, h),
    "y": lambda q, k, h: (1 - q, k, h),
}


def kernel(tok_hbm, gain_ref, gate_hbm, up_hbm, down_hbm, out_hbm,
           x, w, dn, res, hid, own, sb, rb, sd, yl, zl, zh, yf, zf, out,
           tok_sem, w_sem, d_sem, out_sem, x_sem, pair_sem, sd_sem, rs):
    dp, t = lax.axis_index("dp"), lax.axis_index("tensor")
    hi, z, c = t // 8, lax.rem(t // 2, 4), lax.rem(t, 2)

    def member(q, k, core):
        return (hi if q == 0 else 1 - hi) * 8 + lax.rem(z + k, 4) * 2 + core

    peer = {
        "zp": (dp, member(0, 1, c)),
        "zm": (dp, member(0, 3, c)),
        "y": (dp, member(1, 0, c)),
        "s": (dp, member(0, 0, 1 - c)),
    }
    barrier = pltpu.get_barrier_semaphore()
    for link in ("y", "zp", "zm", "s"):
        pl.semaphore_signal(barrier, inc=1, device_id=peer[link], device_id_type=MESH)

    tok_copy = pltpu.make_async_copy(tok_hbm, res.at[c], tok_sem)
    tok_copy.start()
    for j in range(7):
        for part, source in enumerate((gate_hbm, up_hbm)):
            pltpu.make_async_copy(
                source.at[:, pl.ds(j * 128, 128)], w.at[:, pl.ds(j * 256 + part * 128, 128)], w_sem).start()

    count = [0]

    def remote(link, source, dst, sem):
        i = count[0]
        count[0] += 1
        return pltpu.make_async_remote_copy(
            src_ref=source, dst_ref=dst, send_sem=sem, recv_sem=rs.at[i],
            device_id=peer[link], device_id_type=MESH)

    def quarter(q, k, i):
        return x.at[UNIT[q, k, i // 2], i % 2, c]

    def gather(link, source, dst):
        return [remote(link, quarter(*source, i), quarter(*dst, i), x_sem) for i in range(4)]

    zp0, zm0, y0 = gather("zp", (0, 0), (0, 3)), gather("zm", (0, 0), (0, 1)), gather("y", (0, 0), (1, 0))
    zp2 = [remote("zp", quarter(0, 3, i), quarter(0, 2, i), x_sem) for i in (0, 1)]
    zm2 = [remote("zm", quarter(0, 1, i), quarter(0, 2, i), x_sem) for i in (3, 2)]
    zpp, zmp, y2 = gather("zp", (1, 0), (1, 3)), gather("zm", (1, 0), (1, 1)), gather("y", (0, 2), (1, 2))
    sib = {u: remote("s", x.at[UNIT[u], :, c], x.at[UNIT[u], :, c], x_sem) for u in UNITS}

    def rows(lo, n):
        return pl.ds(lo * 64, n * 64)

    pairs, leaf = {}, {}
    for name, (lo, n) in CHUNKS.items():
        at = rows(lo, n)
        pairs[name] = [remote("s", sb.at[pl.ds(a, m), at], rb.at[pl.ds(a, m), at], pair_sem) for a, m in ((0, 3), (3, 5))]
        leaf[name] = {
            "y": remote("y", sd.at[DEST[1, 2], at], yl.at[at], sd_sem),
            "zp": remote("zp", sd.at[DEST[1, 1], at], zl.at[0, at], sd_sem),
            "zm": remote("zm", sd.at[DEST[1, 3], at], zl.at[1, at], sd_sem),
        }
    half, across, last = {}, {}, {}
    for name, (lo, n) in PIECES.items():
        at = rows(lo, n)
        half[name] = {
            "zp": remote("zp", sd.at[DEST[0, 2], at, pl.ds(0, 128)], zh.at[0, at], sd_sem),
            "zm": remote("zm", sd.at[DEST[0, 2], at, pl.ds(128, 128)], zh.at[1, at], sd_sem),
        }
        across[name] = {"y": remote("y", sd.at[DEST[1, 0], at], yf.at[at], sd_sem)}
        last[name] = {
            "zp": remote("zp", sd.at[DEST[0, 1], at], zf.at[0, at], sd_sem),
            "zm": remote("zm", sd.at[DEST[0, 3], at], zf.at[1, at], sd_sem),
        }

    waited = set()

    def arrived(copy):
        if id(copy) not in waited:
            waited.add(id(copy))
            copy.wait_recv()

    def seen(messages, link, unit, table):
        s = UNIT[SEEN[link](*UNITS[unit])]
        for name, (lo, n) in table.items():
            if lo <= s < lo + n:
                arrived(messages[name][link])
        return rows(s, 1)

    res[1 - c] = jnp.zeros((4, 16, D), BF16)
    tok_copy.wait()
    gain = gain_ref[...]
    for i in range(4):
        wide = res[c, i].astype(F32)
        square_mean = jnp.mean(wide * wide, axis=1, keepdims=True)
        normed = wide * gain / jnp.sqrt(square_mean + 1e-05)
        x[i // 2, i % 2, c] = normed.astype(BF16)
    pl.semaphore_wait(barrier, 4)

    sib[0, 0, 0].start()
    sib[0, 0, 1].start()
    for i in range(3):
        zp0[i].start()
        zm0[3 - i].start()
        y0[i].start()
    y0[3].start()
    for r, (q, k) in enumerate(DESTS):
        for part, core in enumerate((1 - c, c)):
            col = pl.multiple_of(member(q, k, core) * COLS, COLS)
            pltpu.make_async_copy(
                down_hbm.at[:, pl.ds(col, COLS)], dn.at[:, pl.ds((2 * r + part) * COLS, COLS)], d_sem).start()

    def dot_in(lo, n):
        both = jnp.dot(x[pl.ds(lo, n)].reshape(n * 64, D), w[...], preferred_element_type=F32)
        for j in range(7):
            gate, up = both[:, j * 256:j * 256 + 128], both[:, j * 256 + 128:j * 256 + 256]
            hid[rows(lo, n), pl.ds(j * 128, 128)] = (gate / (1.0 + jnp.exp(-gate)) * up).astype(BF16)

    def dot_out(lo, n, first, end):
        part = jnp.dot(hid[rows(lo, n)], dn[:, pl.ds(first * 512, (end - first) * 512)], preferred_element_type=F32)
        for r in range(first, end):
            for side in range(2):
                at = (r - first) * 512 + side * 256
                value = part[:, at:at + 256]
                if lo == 0:
                    core = (1 - c, c)[side]
                    col = pl.multiple_of(member(*DESTS[r], core) * COLS, COLS)
                    add = [res[kk, i, :, pl.ds(col, COLS)].astype(F32) for i in range(4) for kk in range(2)]
                    value = value + jnp.concatenate(add, axis=0)
                if side == 0:
                    sb[r, rows(lo, n)] = value.astype(BF16)
                else:
                    own[r, rows(lo, n)] = value

    def chip_sum(r, unit):
        return own[r, rows(unit, 1)] + rb[r, rows(unit, 1)].astype(F32)

    def send_leaf(name, links=("y", "zp", "zm")):
        lo, n = CHUNKS[name]
        arrived(pairs[name][0])
        for link in links:
            r = DEST[{"y": (1, 2), "zp": (1, 1), "zm": (1, 3)}[link]]
            for unit in range(lo, lo + n):
                sd[r, rows(unit, 1)] = chip_sum(r, unit).astype(BF16)
            leaf[name][link].start()

    def pair_rest(lo, n):
        for name, (a, m) in CHUNKS.items():
            if a < lo + n and lo < a + m:
                arrived(pairs[name][1])

    def send_half(name):
        lo, n = PIECES[name]
        pair_rest(lo, n)
        r = DEST[0, 2]
        for unit in range(lo, lo + n):
            got = seen(leaf, "y", unit, CHUNKS)
            sd[r, rows(unit, 1)] = (chip_sum(r, unit) + yl[got].astype(F32)).astype(BF16)
        half[name]["zp"].start()
        half[name]["zm"].start()

    def send_across(name):
        lo, n = PIECES[name]
        pair_rest(lo, n)
        r = DEST[1, 0]
        for unit in range(lo, lo + n):
            value = chip_sum(r, unit)
            value = value + zl[0, seen(leaf, "zp", unit, CHUNKS)].astype(F32)
            value = value + zl[1, seen(leaf, "zm", unit, CHUNKS)].astype(F32)
            sd[r, rows(unit, 1)] = value.astype(BF16)
        across[name]["y"].start()

    def send_last(name):
        lo, n = PIECES[name]
        for link, dest, side in (("zp", (0, 1), 0), ("zm", (0, 3), 1)):
            r = DEST[dest]
            for unit in range(lo, lo + n):
                value = chip_sum(r, unit)
                got = zh[side, seen(half, link, unit, PIECES)].astype(F32)
                keep = (1 - side) * 128
                sd[r, rows(unit, 1), pl.ds(side * 128, 128)] = (value[:, side * 128:side * 128 + 128] + got).astype(BF16)
                sd[r, rows(unit, 1), pl.ds(keep, 128)] = value[:, keep:keep + 128].astype(BF16)
            last[name][link].start()

    out_copies = []

    def finish(unit):
        q, k, h = UNITS[unit]
        value = chip_sum(DEST[0, 0], unit)
        value = value + yf[seen(across, "y", unit, PIECES)].astype(F32)
        value = value + zf[0, seen(last, "zp", unit, PIECES)].astype(F32)
        value = value + zf[1, seen(last, "zm", unit, PIECES)].astype(F32)
        ordered = [value[i * 32 + core * 16:i * 32 + core * 16 + 16] for core in range(2) for i in range(2)]
        out[rows(unit, 1)] = jnp.concatenate(ordered, axis=0).astype(BF16)
        for core in range(2):
            at = pl.multiple_of(member(q, k, core) * 64 + h * 32, 32)
            copy = pltpu.make_async_copy(
                out.at[pl.ds(unit * 64 + core * 32, 32)], out_hbm.at[pl.ds(at, 32)], out_sem)
            copy.start()
            out_copies.append(copy)

    def exchange(*units):
        for unit in units:
            sib[unit].start()

    def have(*units):
        for unit in units:
            arrived(sib[unit])

    def all_sent(ref, sem):
        pltpu.make_async_remote_copy(
            src_ref=ref, dst_ref=ref, send_sem=sem, recv_sem=rs.at[0],
            device_id=peer["s"], device_id_type=MESH).wait_send()

    have((0, 0, 0), (0, 0, 1))
    pltpu.make_async_copy(w, w, w_sem).wait()
    dot_in(0, 2)
    arrived(zp0[0])
    zp2[0].start()
    arrived(zm0[3])
    zm2[0].start()
    pltpu.make_async_copy(dn, dn, d_sem).wait()
    dot_out(0, 2, 0, 3)
    pairs["A"][0].start()
    dot_out(0, 2, 3, 8)
    pairs["A"][1].start()
    arrived(zp0[1])
    zp2[1].start()
    zp0[3].start()
    exchange((0, 3, 0))
    arrived(zm0[2])
    zm2[1].start()
    zm0[0].start()
    exchange((0, 1, 1))
    for i in range(2):
        arrived(y0[i])
        zpp[i].start()
        zmp[i].start()
    exchange((1, 0, 0))
    have((0, 3, 0), (0, 1, 1), (1, 0, 0))
    dot_in(2, 3)
    send_leaf("A", ("y",))
    dot_out(2, 3, 0, 3)
    pairs["B"][0].start()
    for i in range(2, 4):
        arrived(y0[i])
        zpp[i].start()
        zmp[i].start()
    exchange((1, 0, 1))
    arrived(zp2[0])
    y2[0].start()
    arrived(zm2[0])
    y2[3].start()
    dot_out(2, 3, 3, 8)
    pairs["B"][1].start()
    send_leaf("A", ("zp", "zm"))
    arrived(zp2[1])
    y2[1].start()
    exchange((0, 2, 0))
    arrived(zm2[1])
    y2[2].start()
    exchange((0, 2, 1))
    send_leaf("B")
    have((1, 0, 1), (0, 2, 0), (0, 2, 1))
    dot_in(5, 3)
    arrived(zp0[2])
    arrived(zp0[3])
    exchange((0, 3, 1))
    arrived(zm0[1])
    arrived(zm0[0])
    exchange((0, 1, 0))
    dot_out(5, 3, 0, 3)
    pairs["C"][0].start()
    dot_out(5, 3, 3, 8)
    pairs["C"][1].start()
    have((0, 3, 1), (0, 1, 0))
    dot_in(8, 2)
    send_leaf("C")
    for copies, unit in ((zpp, (1, 3, 0)), (zmp, (1, 1, 0))):
        arrived(copies[0])
        arrived(copies[1])
        exchange(unit)
    dot_out(8, 2, 0, 3)
    pairs["D"][0].start()
    dot_out(8, 2, 3, 8)
    pairs["D"][1].start()
    have((1, 3, 0), (1, 1, 0))
    dot_in(10, 2)
    send_leaf("D")
    for h in range(2):
        arrived(y2[2 * h])
        arrived(y2[2 * h + 1])
        exchange((1, 2, h))
    have((1, 2, 0), (1, 2, 1))
    dot_in(12, 2)
    for copies, unit in ((zpp, (1, 3, 1)), (zmp, (1, 1, 1))):
        arrived(copies[2])
        arrived(copies[3])
        exchange(unit)
    dot_out(10, 4, 0, 3)
    pairs["E"][0].start()
    have((1, 3, 1), (1, 1, 1))
    dot_in(14, 2)
    send_leaf("E")
    dot_out(14, 2, 0, 3)
    pairs["F"][0].start()
    dot_out(10, 4, 3, 8)
    pairs["E"][1].start()
    send_leaf("F")
    dot_out(14, 2, 3, 8)
    pairs["F"][1].start()
    send_half("C")
    send_half("E")
    send_across("D")
    send_half("AB")
    send_half("D")
    send_half("F")
    send_across("AB")
    send_across("F")
    send_across("E")
    send_across("C")
    for name in ("F", "D", "AB", "E", "C"):
        send_last(name)
    for name in ("F", "D", "AB", "E", "C"):
        lo, n = PIECES[name]
        for unit in range(lo, lo + n):
            finish(unit)
    all_sent(x.at[pl.ds(0, 15)], x_sem)
    all_sent(sb, pair_sem)
    all_sent(sd, sd_sem)
    pltpu.make_async_copy(out, out_hbm, out_sem).wait()


N_REMOTE = 28 + 16 + 6 * 5 + 5 * 5
ANY, VMEM = pl.BlockSpec(memory_space=pl.ANY), pl.BlockSpec(memory_space=pltpu.VMEM)


def on_device(tokens, norm_gain, gate_weight, up_weight, down_weight):
    return pl.pallas_call(
        kernel,
        out_shape=jax.ShapeDtypeStruct((ROWS, COLS), BF16),
        in_specs=[ANY, VMEM, ANY, ANY, ANY],
        out_specs=ANY,
        scratch_shapes=[
            pltpu.VMEM((16, 2, 2, 16, D), BF16),
            pltpu.VMEM((D, 2 * F), BF16),
            pltpu.VMEM((F, D), BF16),
            pltpu.VMEM((2, 4, 16, D), BF16),
            pltpu.VMEM((ROWS, F), BF16),
            pltpu.VMEM((8, ROWS, COLS), F32),
            pltpu.VMEM((8, ROWS, COLS), BF16),
            pltpu.VMEM((8, ROWS, COLS), BF16),
            pltpu.VMEM((7, ROWS, COLS), BF16),
            pltpu.VMEM((ROWS, COLS), BF16),
            pltpu.VMEM((2, ROWS, COLS), BF16),
            pltpu.VMEM((2, ROWS, 128), BF16),
            pltpu.VMEM((ROWS, COLS), BF16),
            pltpu.VMEM((2, ROWS, COLS), BF16),
            pltpu.VMEM((ROWS, COLS), BF16),
            pltpu.SemaphoreType.DMA,
            pltpu.SemaphoreType.DMA,
            pltpu.SemaphoreType.DMA,
            pltpu.SemaphoreType.DMA,
            pltpu.SemaphoreType.DMA,
            pltpu.SemaphoreType.DMA,
            pltpu.SemaphoreType.DMA,
            pltpu.SemaphoreType.DMA((N_REMOTE,)),
        ],
        compiler_params=pltpu.CompilerParams(
            collective_id=0, has_side_effects=True, vmem_limit_bytes=67043328),
    )(tokens.reshape(4, 16, D), norm_gain.reshape(1, D), gate_weight, up_weight, down_weight)


def solution(mesh):
    return jax.shard_map(
        on_device,
        mesh=mesh,
        in_specs=(
            P(("dp", "tensor"), None),
            P(),
            P(None, "tensor"),
            P(None, "tensor"),
            P("tensor", None),
        ),
        out_specs=P("dp", "tensor"),
        check_vma=False,
    )
```

```python
import jax
import jax.numpy as jnp
from jax import lax
from jax.experimental import pallas as pl
from jax.experimental.pallas import tpu as pltpu
from jax.sharding import PartitionSpec as P

MESH = pl.DeviceIdType.MESH
F32, BF16 = jnp.float32, jnp.bfloat16
D, F, ROWS, COLS = 4096, 896, 1024, 256

UNITS = [(0, 0, 0), (0, 0, 1),
         (0, 3, 0), (0, 1, 1), (1, 0, 0),
         (1, 0, 1), (0, 2, 0), (0, 2, 1),
         (0, 3, 1), (0, 1, 0),
         (1, 3, 0), (1, 1, 0), (1, 2, 0), (1, 2, 1),
         (1, 3, 1), (1, 1, 1)]
UNIT = {b: i for i, b in enumerate(UNITS)}
QUARTERED = [(0, 3, 0), (0, 1, 1), (1, 0, 0), (1, 3, 1), (1, 1, 1)]
CHUNKS = {"A": (0, 2), "B": (2, 3), "C": (5, 3), "D": (8, 2), "E": (10, 4), "F": (14, 2)}
DESTS = [(1, 2), (1, 1), (1, 3), (0, 2), (1, 0), (0, 1), (0, 3), (0, 0)]
DEST = {b: i for i, b in enumerate(DESTS)}
HALF = [[(0, 0, 0), (0, 0, 1), (1, 0, 0), (1, 0, 1)],
        [(1, 2, 0), (1, 2, 1), (1, 3, 0), (1, 1, 0), (0, 2, 0), (0, 2, 1), (0, 3, 0), (0, 1, 0)],
        [(0, 3, 1), (0, 1, 1), (1, 3, 1), (1, 1, 1)]]
ACROSS = [[(0, k, h) for k in range(4) for h in range(2)], [(1, k, 0) for k in range(4)], [(1, k, 1) for k in range(4)]]
LAST = {link: [[(0, p, 0), (0, p, 1)],
               [(1, p, 0), (0, m, 0), (0, m, 1), (1, 2, 0), (1, m, 0), (0, 0, 0), (0, 2, 0), (1, 0, 0)],
               [(1, p, 1), (1, m, 1), (0, 0, 1), (0, 2, 1), (1, 0, 1), (1, 2, 1)]]
        for link, p, m in (("zp", 3, 1), ("zm", 1, 3))}
SEEN = {
    "zp": lambda q, k, h: (q, (k + 1) % 4, h),
    "zm": lambda q, k, h: (q, (k + 3) % 4, h),
    "y": lambda q, k, h: (1 - q, k, h),
}


def kernel(tok_hbm, gain_ref, gate_hbm, up_hbm, down_hbm, out,
           x, w, dn, res, hid, own, sb, rb, sd, yl, zl, zh, yf, zf,
           tok_sem, w_sem, d_sem, x_sem, pair_sem, sd_sem, rs):
    dp, t = lax.axis_index("dp"), lax.axis_index("tensor")
    hi, z, c = t // 8, lax.rem(t // 2, 4), lax.rem(t, 2)

    def member(q, k, core):
        return (hi if q == 0 else 1 - hi) * 8 + lax.rem(z + k, 4) * 2 + core

    peer = {
        "zp": (dp, member(0, 1, c)),
        "zm": (dp, member(0, 3, c)),
        "y": (dp, member(1, 0, c)),
        "s": (dp, member(0, 0, 1 - c)),
    }
    barrier = pltpu.get_barrier_semaphore()
    for link in ("y", "zp", "zm", "s"):
        pl.semaphore_signal(barrier, inc=1, device_id=peer[link], device_id_type=MESH)

    tok_copy = pltpu.make_async_copy(tok_hbm, res.at[c], tok_sem)
    tok_copy.start()
    count = [0]

    def remote(link, source, dst, sem):
        i = count[0]
        count[0] += 1
        return pltpu.make_async_remote_copy(
            src_ref=source, dst_ref=dst, send_sem=sem, recv_sem=rs.at[i],
            device_id=peer[link], device_id_type=MESH)

    def quarter(q, k, i):
        return x.at[UNIT[q, k, i // 2], i % 2, c]

    def gather(link, source, dst):
        return [remote(link, quarter(*source, i), quarter(*dst, i), x_sem) for i in range(4)]

    zp0, zm0, y0 = gather("zp", (0, 0), (0, 3)), gather("zm", (0, 0), (0, 1)), gather("y", (0, 0), (1, 0))
    zp2 = [remote("zp", quarter(0, 3, i), quarter(0, 2, i), x_sem) for i in (0, 1)]
    zm2 = [remote("zm", quarter(0, 1, i), quarter(0, 2, i), x_sem) for i in (3, 2)]
    zpp, zmp, y2 = gather("zp", (1, 0), (1, 3)), gather("zm", (1, 0), (1, 1)), gather("y", (0, 2), (1, 2))
    sib = {}
    for u in UNITS:
        if u in QUARTERED:
            sib[u] = [remote("s", x.at[UNIT[u], i, c], x.at[UNIT[u], i, c], x_sem) for i in range(2)]
        else:
            sib[u] = [remote("s", x.at[UNIT[u], :, c], x.at[UNIT[u], :, c], x_sem)]

    def rows(lo, n):
        return pl.ds(lo * 64, n * 64)

    pairs, leaf = {}, {}
    for name, (lo, n) in CHUNKS.items():
        at = rows(lo, n)
        pairs[name] = [remote("s", sb.at[pl.ds(a, m), at], rb.at[pl.ds(a, m), at], pair_sem) for a, m in ((0, 3), (3, 5))]
        leaf[name] = {
            "y": remote("y", sd.at[DEST[1, 2], at], yl.at[at], sd_sem),
            "zp": remote("zp", sd.at[DEST[1, 1], at], zl.at[0, at], sd_sem),
            "zm": remote("zm", sd.at[DEST[1, 3], at], zl.at[1, at], sd_sem),
        }
    def pieces(orders, make):
        copies, where, at = [], {}, 0
        for i, units in enumerate(orders):
            copies.append(make(rows(at, len(units))))
            for unit in units:
                where[unit] = (i, at)
                at += 1
        return copies, where

    half = {}
    for link, side in (("zp", 0), ("zm", 1)):
        half[link] = pieces(HALF, lambda at: remote(
            link, sd.at[DEST[0, 2], at, pl.ds(side * 128, 128)], zh.at[side, at], sd_sem))
    across = {"y": pieces(ACROSS, lambda at: remote("y", sd.at[DEST[1, 0], at], yf.at[at], sd_sem))}
    last = {}
    for link, side, k in (("zp", 0, 1), ("zm", 1, 3)):
        last[link] = pieces(LAST[link], lambda at: remote(link, sd.at[DEST[0, k], at], zf.at[side, at], sd_sem))

    waited = set()

    def arrived(copy):
        if id(copy) not in waited:
            waited.add(id(copy))
            copy.wait_recv()

    def seen_leaf(link, unit):
        at = UNIT[SEEN[link](*unit)]
        for name, (lo, n) in CHUNKS.items():
            if lo <= at < lo + n:
                arrived(leaf[name][link])
        return rows(at, 1)

    def seen(messages, link, unit):
        copies, where = messages[link]
        i, at = where[SEEN[link](*unit)]
        arrived(copies[i])
        return rows(at, 1)

    def exchange(*units):
        for unit in units:
            for copy in sib[unit]:
                copy.start()

    res[1 - c] = jnp.zeros((4, 16, D), BF16)
    tok_copy.wait()
    for j in range(7):
        for part, source in enumerate((gate_hbm, up_hbm)):
            pltpu.make_async_copy(
                source.at[:, pl.ds(j * 128, 128)], w.at[:, pl.ds(j * 256 + part * 128, 128)], w_sem).start()
    gain = gain_ref[...]
    for i in range(4):
        wide = res[c, i].astype(F32)
        square_mean = jnp.mean(wide * wide, axis=1, keepdims=True)
        normed = wide * gain / jnp.sqrt(square_mean + 1e-05)
        x[i // 2, i % 2, c] = normed.astype(BF16)
    pl.semaphore_wait(barrier, 4)

    exchange((0, 0, 0), (0, 0, 1))
    for i in range(3):
        zp0[i].start()
        zm0[3 - i].start()
        y0[i].start()
    y0[3].start()
    for r, (q, k) in enumerate(DESTS):
        for part, core in enumerate((1 - c, c)):
            col = pl.multiple_of(member(q, k, core) * COLS, COLS)
            pltpu.make_async_copy(
                down_hbm.at[:, pl.ds(col, COLS)], dn.at[:, pl.ds((2 * r + part) * COLS, COLS)], d_sem).start()

    def dot_in(lo, n):
        both = jnp.dot(x[pl.ds(lo, n)].reshape(n * 64, D), w[...], preferred_element_type=F32)
        for j in range(7):
            gate, up = both[:, j * 256:j * 256 + 128], both[:, j * 256 + 128:j * 256 + 256]
            hid[rows(lo, n), pl.ds(j * 128, 128)] = (gate / (1.0 + jnp.exp(-gate)) * up).astype(BF16)

    def dot_out(lo, n, first, end):
        part = jnp.dot(hid[rows(lo, n)], dn[:, pl.ds(first * 512, (end - first) * 512)], preferred_element_type=F32)
        for r in range(first, end):
            for side in range(2):
                at = (r - first) * 512 + side * 256
                value = part[:, at:at + 256]
                if lo == 0:
                    core = (1 - c, c)[side]
                    col = pl.multiple_of(member(*DESTS[r], core) * COLS, COLS)
                    add = [res[kk, i, :, pl.ds(col, COLS)].astype(F32) for i in range(4) for kk in range(2)]
                    value = value + jnp.concatenate(add, axis=0)
                if side == 0:
                    sb[r, rows(lo, n)] = value.astype(BF16)
                else:
                    own[r, rows(lo, n)] = value

    def chip_sum(r, unit, rest=True):
        at = UNIT[unit]
        for name, (lo, n) in CHUNKS.items():
            if lo <= at < lo + n:
                arrived(pairs[name][1 if rest else 0])
        return own[r, rows(at, 1)] + rb[r, rows(at, 1)].astype(F32)

    def send_leaf(name, links=("y", "zp", "zm")):
        lo, n = CHUNKS[name]
        for link in links:
            r = DEST[{"y": (1, 2), "zp": (1, 1), "zm": (1, 3)}[link]]
            for unit in range(lo, lo + n):
                sd[r, rows(unit, 1)] = chip_sum(r, UNITS[unit], False).astype(BF16)
            leaf[name][link].start()

    def send_half(i):
        r = DEST[0, 2]
        where = half["zp"][1]
        for unit in HALF[i]:
            got = seen_leaf("y", unit)
            sd[r, rows(where[unit][1], 1)] = (chip_sum(r, unit) + yl[got].astype(F32)).astype(BF16)
        half["zp"][0][i].start()
        half["zm"][0][i].start()

    def send_across(i):
        r = DEST[1, 0]
        copies, where = across["y"]
        for unit in ACROSS[i]:
            value = chip_sum(r, unit)
            value = value + zl[0, seen_leaf("zp", unit)].astype(F32)
            value = value + zl[1, seen_leaf("zm", unit)].astype(F32)
            sd[r, rows(where[unit][1], 1)] = value.astype(BF16)
        copies[i].start()

    def send_last(i):
        for link, side, k in (("zp", 0, 1), ("zm", 1, 3)):
            r = DEST[0, k]
            copies, where = last[link]
            for unit in LAST[link][i]:
                value = chip_sum(r, unit)
                got = zh[side, seen(half, link, unit)].astype(F32)
                keep = (1 - side) * 128
                at = rows(where[unit][1], 1)
                sd[r, at, pl.ds(side * 128, 128)] = (value[:, side * 128:side * 128 + 128] + got).astype(BF16)
                sd[r, at, pl.ds(keep, 128)] = value[:, keep:keep + 128].astype(BF16)
            copies[i].start()

    def finish(unit):
        q, k, h = unit
        value = chip_sum(DEST[0, 0], unit)
        value = value + yf[seen(across, "y", unit)].astype(F32)
        value = value + zf[0, seen(last, "zp", unit)].astype(F32)
        value = value + zf[1, seen(last, "zm", unit)].astype(F32)
        for core in range(2):
            at = pl.multiple_of(member(q, k, core) * 64 + h * 32, 32)
            ordered = [value[i * 32 + core * 16:i * 32 + core * 16 + 16] for i in range(2)]
            out[pl.ds(at, 32)] = jnp.concatenate(ordered, axis=0).astype(BF16)

    def have(*units):
        for unit in units:
            for copy in sib[unit]:
                arrived(copy)

    def all_sent(ref, sem):
        pltpu.make_async_remote_copy(
            src_ref=ref, dst_ref=ref, send_sem=sem, recv_sem=rs.at[0],
            device_id=peer["s"], device_id_type=MESH).wait_send()

    have((0, 0, 0), (0, 0, 1))
    pltpu.make_async_copy(w, w, w_sem).wait()
    dot_in(0, 2)
    arrived(zp0[0])
    zp2[0].start()
    sib[0, 3, 0][0].start()
    arrived(zm0[3])
    zm2[0].start()
    sib[0, 1, 1][1].start()
    arrived(y0[0])
    sib[1, 0, 0][0].start()
    pltpu.make_async_copy(dn, dn, d_sem).wait()
    dot_out(0, 2, 0, 3)
    pairs["A"][0].start()
    dot_out(0, 2, 3, 8)
    pairs["A"][1].start()
    arrived(zp0[1])
    zp2[1].start()
    zp0[3].start()
    sib[0, 3, 0][1].start()
    arrived(zm0[2])
    zm2[1].start()
    zm0[0].start()
    sib[0, 1, 1][0].start()
    arrived(y0[1])
    sib[1, 0, 0][1].start()
    for i in range(2):
        zpp[i].start()
        zmp[i].start()
    have((0, 3, 0), (0, 1, 1), (1, 0, 0))
    dot_in(2, 3)
    send_leaf("A", ("y",))
    dot_out(2, 3, 0, 3)
    pairs["B"][0].start()
    for i in range(2, 4):
        arrived(y0[i])
        zpp[i].start()
        zmp[i].start()
    exchange((1, 0, 1))
    arrived(zp2[0])
    y2[0].start()
    arrived(zm2[0])
    y2[3].start()
    dot_out(2, 3, 3, 8)
    pairs["B"][1].start()
    send_leaf("A", ("zp", "zm"))
    arrived(zp2[1])
    y2[1].start()
    exchange((0, 2, 0))
    arrived(zm2[1])
    y2[2].start()
    exchange((0, 2, 1))
    send_leaf("B")
    have((1, 0, 1), (0, 2, 0), (0, 2, 1))
    dot_in(5, 3)
    arrived(zp0[2])
    arrived(zp0[3])
    exchange((0, 3, 1))
    arrived(zm0[1])
    arrived(zm0[0])
    exchange((0, 1, 0))
    dot_out(5, 3, 0, 3)
    pairs["C"][0].start()
    dot_out(5, 3, 3, 8)
    pairs["C"][1].start()
    have((0, 3, 1), (0, 1, 0))
    dot_in(8, 2)
    send_leaf("C")
    for copies, unit in ((zpp, (1, 3, 0)), (zmp, (1, 1, 0))):
        arrived(copies[0])
        arrived(copies[1])
        exchange(unit)
    dot_out(8, 2, 0, 3)
    pairs["D"][0].start()
    dot_out(8, 2, 3, 8)
    pairs["D"][1].start()
    have((1, 3, 0), (1, 1, 0))
    dot_in(10, 2)
    send_leaf("D")
    for h in range(2):
        arrived(y2[2 * h])
        arrived(y2[2 * h + 1])
        exchange((1, 2, h))
    have((1, 2, 0), (1, 2, 1))
    dot_in(12, 2)
    for i in (2, 3):
        for copies, unit in ((zpp, (1, 3, 1)), (zmp, (1, 1, 1))):
            arrived(copies[i])
            sib[unit][i - 2].start()
    dot_out(10, 4, 0, 3)
    pairs["E"][0].start()
    send_half(0)
    dot_out(10, 4, 3, 8)
    pairs["E"][1].start()
    send_leaf("E")
    send_across(0)
    have((1, 3, 1), (1, 1, 1))
    dot_in(14, 2)
    send_last(0)
    dot_out(14, 2, 0, 3)
    pairs["F"][0].start()
    send_half(1)
    dot_out(14, 2, 3, 8)
    pairs["F"][1].start()
    send_leaf("F")
    send_across(1)
    send_last(1)
    send_half(2)
    send_across(2)
    send_last(2)
    piece = {u: max(last[link][1][SEEN[link](*u)][0] for link in ("zp", "zm")) for u in UNITS}
    for unit in sorted(UNITS, key=lambda u: piece[u]):
        finish(unit)
    all_sent(x.at[pl.ds(0, 15)], x_sem)
    all_sent(sb, pair_sem)
    all_sent(sd, sd_sem)


N_REMOTE = 28 + 16 + 5 + 6 * 5 + 15
ANY, VMEM = pl.BlockSpec(memory_space=pl.ANY), pl.BlockSpec(memory_space=pltpu.VMEM)


def on_device(tokens, norm_gain, gate_weight, up_weight, down_weight):
    return pl.pallas_call(
        kernel,
        out_shape=pltpu.VMEM((ROWS, COLS), BF16),
        in_specs=[ANY, VMEM, ANY, ANY, ANY],
        out_specs=VMEM,
        scratch_shapes=[
            pltpu.VMEM((16, 2, 2, 16, D), BF16),
            pltpu.VMEM((D, 2 * F), BF16),
            pltpu.VMEM((F, D), BF16),
            pltpu.VMEM((2, 4, 16, D), BF16),
            pltpu.VMEM((ROWS, F), BF16),
            pltpu.VMEM((8, ROWS, COLS), F32),
            pltpu.VMEM((8, ROWS, COLS), BF16),
            pltpu.VMEM((8, ROWS, COLS), BF16),
            pltpu.VMEM((7, ROWS, COLS), BF16),
            pltpu.VMEM((ROWS, COLS), BF16),
            pltpu.VMEM((2, ROWS, COLS), BF16),
            pltpu.VMEM((2, ROWS, 128), BF16),
            pltpu.VMEM((ROWS, COLS), BF16),
            pltpu.VMEM((2, ROWS, COLS), BF16),
            pltpu.SemaphoreType.DMA,
            pltpu.SemaphoreType.DMA,
            pltpu.SemaphoreType.DMA,
            pltpu.SemaphoreType.DMA,
            pltpu.SemaphoreType.DMA,
            pltpu.SemaphoreType.DMA,
            pltpu.SemaphoreType.DMA((N_REMOTE,)),
        ],
        compiler_params=pltpu.CompilerParams(
            collective_id=0, has_side_effects=True, vmem_limit_bytes=62 * 2**20),
    )(tokens.reshape(4, 16, D), norm_gain.reshape(1, D), gate_weight, up_weight, down_weight)


def solution(mesh):
    return jax.shard_map(
        on_device,
        mesh=mesh,
        in_specs=(
            P(("dp", "tensor"), None),
            P(),
            P(None, "tensor"),
            P(None, "tensor"),
            P("tensor", None),
        ),
        out_specs=P("dp", "tensor"),
        check_vma=False,
    )
```

```python
import jax
import jax.numpy as jnp
from jax import lax
from jax.experimental import pallas as pl
from jax.experimental.pallas import tpu as pltpu
from jax.sharding import PartitionSpec as P

MESH = pl.DeviceIdType.MESH
F32, BF16 = jnp.float32, jnp.bfloat16
D, F, ROWS, COLS = 4096, 896, 1024, 256

UNITS = [(0, 0, 0), (0, 0, 1),
         (0, 3, 0), (0, 1, 1), (1, 0, 0),
         (1, 0, 1), (0, 2, 0), (0, 2, 1),
         (0, 3, 1), (0, 1, 0),
         (1, 3, 0), (1, 1, 0),
         (1, 2, 0), (1, 2, 1),
         (1, 3, 1), (1, 1, 1)]
UNIT = {b: i for i, b in enumerate(UNITS)}
QUARTERED = [(0, 3, 0), (0, 1, 1), (1, 0, 0), (1, 3, 1), (1, 1, 1)]
CHUNKS = {"A": (0, 2), "B": (2, 3), "C": (5, 3), "D": (8, 2), "E": (10, 2), "G": (12, 2), "K": (14, 2)}
ACROSS_Y = "G"
DESTS = [(1, 2), (1, 1), (1, 3), (0, 2), (1, 0), (0, 1), (0, 3), (0, 0)]
DEST = {b: i for i, b in enumerate(DESTS)}
HALF = [[(0, 0, 0), (0, 0, 1), (1, 0, 0), (1, 0, 1)],
        [(1, 3, 0), (1, 1, 0), (0, 3, 0), (0, 1, 0)],
        [(1, 2, 0), (1, 2, 1), (0, 2, 0), (0, 2, 1)],
        [(1, 3, 1), (1, 1, 1), (0, 3, 1), (0, 1, 1)]]
ACROSS = [[(0, 1, 0), (0, 1, 1), (0, 3, 0), (0, 3, 1)], [(0, 0, 0), (0, 0, 1), (0, 2, 0), (0, 2, 1)],
          [(1, k, 0) for k in range(4)], [(1, k, 1) for k in range(4)]]
LAST = {link: [[(0, p, 0), (0, p, 1), (1, p, 0)],
               [(0, 0, 0), (1, 0, 0)],
               [(1, p, 1), (1, 2, 0)],
               [(0, m, 0), (0, m, 1), (1, m, 0), (1, m, 1), (0, 2, 0)],
               [(0, 0, 1), (0, 2, 1), (1, 0, 1), (1, 2, 1)]]
        for link, p, m in (("zp", 3, 1), ("zm", 1, 3))}
SEEN = {
    "zp": lambda q, k, h: (q, (k + 1) % 4, h),
    "zm": lambda q, k, h: (q, (k + 3) % 4, h),
    "y": lambda q, k, h: (1 - q, k, h),
}


def kernel(tok_hbm, gain_ref, gate_hbm, up_hbm, down_hbm, out,
           x, w, dn, res, hid, own, sb, rb, sd, yl, yp, zl, zh, yf, zf,
           tok_sem, w_sem, d_sem, x_sem, pair_sem, sd_sem, rs):
    dp, t = lax.axis_index("dp"), lax.axis_index("tensor")
    hi, z, c = t // 8, lax.rem(t // 2, 4), lax.rem(t, 2)

    def member(q, k, core):
        return (hi if q == 0 else 1 - hi) * 8 + lax.rem(z + k, 4) * 2 + core

    peer = {
        "zp": (dp, member(0, 1, c)),
        "zm": (dp, member(0, 3, c)),
        "y": (dp, member(1, 0, c)),
        "s": (dp, member(0, 0, 1 - c)),
    }
    barrier = pltpu.get_barrier_semaphore()
    for link in ("y", "zp", "zm", "s"):
        pl.semaphore_signal(barrier, inc=1, device_id=peer[link], device_id_type=MESH)

    tok_copy = pltpu.make_async_copy(tok_hbm, res.at[c], tok_sem)
    tok_copy.start()
    count = [0]

    def remote(link, source, dst, sem):
        i = count[0]
        count[0] += 1
        return pltpu.make_async_remote_copy(
            src_ref=source, dst_ref=dst, send_sem=sem, recv_sem=rs.at[i],
            device_id=peer[link], device_id_type=MESH)

    def quarter(q, k, i):
        return x.at[UNIT[q, k, i // 2], i % 2, c]

    def gather(link, source, dst):
        return [remote(link, quarter(*source, i), quarter(*dst, i), x_sem) for i in range(4)]

    zp0, zm0, y0 = gather("zp", (0, 0), (0, 3)), gather("zm", (0, 0), (0, 1)), gather("y", (0, 0), (1, 0))
    zp2 = [remote("zp", quarter(0, 3, i), quarter(0, 2, i), x_sem) for i in (0, 1)]
    zm2 = [remote("zm", quarter(0, 1, i), quarter(0, 2, i), x_sem) for i in (3, 2)]
    zpp, zmp, y2 = gather("zp", (1, 0), (1, 3)), gather("zm", (1, 0), (1, 1)), gather("y", (0, 2), (1, 2))
    sib = {}
    for u in UNITS:
        if u in QUARTERED:
            sib[u] = [remote("s", x.at[UNIT[u], i, c], x.at[UNIT[u], i, c], x_sem) for i in range(2)]
        else:
            sib[u] = [remote("s", x.at[UNIT[u], :, c], x.at[UNIT[u], :, c], x_sem)]

    def rows(lo, n):
        return pl.ds(lo * 64, n * 64)

    pairs, leaf = {}, {}
    for name, (lo, n) in CHUNKS.items():
        at = rows(lo, n)
        cuts = ((0, 3), (3, 5)) if name in "GK" else ((0, 8),)
        pairs[name] = [remote("s", sb.at[pl.ds(a, m), at], rb.at[pl.ds(a, m), at], pair_sem) for a, m in cuts]
        leaf[name] = {"y": remote("y", sd.at[DEST[1, 2], at], yl.at[at], sd_sem)}
        for link, side, dest in (("zp", 0, (1, 1)), ("zm", 1, (1, 3))):
            if name == ACROSS_Y:
                leaf[name][link] = remote("y", sd.at[DEST[dest], at], yp.at[side], sd_sem)
            else:
                leaf[name][link] = remote(link, sd.at[DEST[dest], at], zl.at[side, at], sd_sem)

    def pieces(orders, make):
        copies, where, at = [], {}, 0
        for i, units in enumerate(orders):
            copies.append(make(rows(at, len(units))))
            for unit in units:
                where[unit] = (i, at)
                at += 1
        return copies, where

    half = {}
    for link, side in (("zp", 0), ("zm", 1)):
        half[link] = pieces(HALF, lambda at: remote(
            link, sd.at[DEST[0, 2], at, pl.ds(side * 128, 128)], zh.at[side, at], sd_sem))
    across = {"y": pieces(ACROSS, lambda at: remote("y", sd.at[DEST[1, 0], at], yf.at[at], sd_sem))}
    last = {}
    for link, side, k in (("zp", 0, 1), ("zm", 1, 3)):
        last[link] = pieces(LAST[link], lambda at: remote(link, sd.at[DEST[0, k], at], zf.at[side, at], sd_sem))

    waited = set()

    def arrived(copy):
        if id(copy) not in waited:
            waited.add(id(copy))
            copy.wait_recv()

    def on_y(unit):
        lo, n = CHUNKS[ACROSS_Y]
        return lo <= UNIT[unit] < lo + n

    def seen_leaf(link, unit):
        at = UNIT[SEEN[link](*unit)]
        for name, (lo, n) in CHUNKS.items():
            if lo <= at < lo + n:
                arrived(leaf[name][link])
        return rows(at, 1)

    def seen(messages, link, unit):
        copies, where = messages[link]
        i, at = where[SEEN[link](*unit)]
        arrived(copies[i])
        return rows(at, 1)

    def exchange(*units):
        for unit in units:
            for copy in sib[unit]:
                copy.start()

    res[1 - c] = jnp.zeros((4, 16, D), BF16)
    tok_copy.wait()
    for j in range(7):
        for part, source in enumerate((gate_hbm, up_hbm)):
            pltpu.make_async_copy(
                source.at[:, pl.ds(j * 128, 128)], w.at[:, pl.ds(j * 256 + part * 128, 128)], w_sem).start()
    gain = gain_ref[...]
    for i in range(4):
        wide = res[c, i].astype(F32)
        square_mean = jnp.mean(wide * wide, axis=1, keepdims=True)
        normed = wide * gain / jnp.sqrt(square_mean + 1e-05)
        x[i // 2, i % 2, c] = normed.astype(BF16)
    pl.semaphore_wait(barrier, 4)

    exchange((0, 0, 0), (0, 0, 1))
    for i in range(3):
        zp0[i].start()
        zm0[3 - i].start()
        y0[i].start()
    y0[3].start()
    for r, (q, k) in enumerate(DESTS):
        for part, core in enumerate((1 - c, c)):
            col = pl.multiple_of(member(q, k, core) * COLS, COLS)
            pltpu.make_async_copy(
                down_hbm.at[:, pl.ds(col, COLS)], dn.at[:, pl.ds((2 * r + part) * COLS, COLS)], d_sem).start()

    def dot_in(lo, n):
        both = jnp.dot(x[pl.ds(lo, n)].reshape(n * 64, D), w[...], preferred_element_type=F32)
        for j in range(7):
            gate, up = both[:, j * 256:j * 256 + 128], both[:, j * 256 + 128:j * 256 + 256]
            hid[rows(lo, n), pl.ds(j * 128, 128)] = (gate / (1.0 + jnp.exp(-gate)) * up).astype(BF16)

    def dot_out(lo, n, first, end):
        part = jnp.dot(hid[rows(lo, n)], dn[:, pl.ds(first * 512, (end - first) * 512)], preferred_element_type=F32)
        for r in range(first, end):
            for side in range(2):
                at = (r - first) * 512 + side * 256
                value = part[:, at:at + 256]
                if lo == 0:
                    core = (1 - c, c)[side]
                    col = pl.multiple_of(member(*DESTS[r], core) * COLS, COLS)
                    add = [res[kk, i, :, pl.ds(col, COLS)].astype(F32) for i in range(4) for kk in range(2)]
                    value = value + jnp.concatenate(add, axis=0)
                if side == 0:
                    sb[r, rows(lo, n)] = value.astype(BF16)
                else:
                    own[r, rows(lo, n)] = value

    def chip_sum(r, unit, rest=True):
        at = UNIT[unit]
        for name, (lo, n) in CHUNKS.items():
            if lo <= at < lo + n:
                arrived(pairs[name][-1 if rest else 0])
        return own[r, rows(at, 1)] + rb[r, rows(at, 1)].astype(F32)

    def send_leaf(name, links=("y", "zp", "zm")):
        lo, n = CHUNKS[name]
        for link in links:
            r = DEST[{"y": (1, 2), "zp": (1, 1), "zm": (1, 3)}[link]]
            for unit in range(lo, lo + n):
                sd[r, rows(unit, 1)] = chip_sum(r, UNITS[unit], False).astype(BF16)
            leaf[name][link].start()

    def send_half(i):
        r = DEST[0, 2]
        where = half["zp"][1]
        for unit in HALF[i]:
            got = seen_leaf("y", unit)
            sd[r, rows(where[unit][1], 1)] = (chip_sum(r, unit) + yl[got].astype(F32)).astype(BF16)
        half["zp"][0][i].start()
        half["zm"][0][i].start()

    def send_across(i):
        r = DEST[1, 0]
        copies, where = across["y"]
        for unit in ACROSS[i]:
            value = chip_sum(r, unit)
            for link, side in (("zp", 0), ("zm", 1)):
                if not on_y(SEEN[link](*unit)):
                    value = value + zl[side, seen_leaf(link, unit)].astype(F32)
            sd[r, rows(where[unit][1], 1)] = value.astype(BF16)
        copies[i].start()

    def send_last(i):
        for link, side, k in (("zp", 0, 1), ("zm", 1, 3)):
            r = DEST[0, k]
            copies, where = last[link]
            for unit in LAST[link][i]:
                value = chip_sum(r, unit)
                theirs = SEEN["y"](*unit)
                if on_y(theirs):
                    arrived(leaf[ACROSS_Y][link])
                    value = value + yp[side, rows(UNIT[theirs] - CHUNKS[ACROSS_Y][0], 1)].astype(F32)
                got = zh[side, seen(half, link, unit)].astype(F32)
                keep = (1 - side) * 128
                at = rows(where[unit][1], 1)
                sd[r, at, pl.ds(side * 128, 128)] = (value[:, side * 128:side * 128 + 128] + got).astype(BF16)
                sd[r, at, pl.ds(keep, 128)] = value[:, keep:keep + 128].astype(BF16)
            copies[i].start()

    def finish(unit):
        q, k, h = unit
        value = chip_sum(DEST[0, 0], unit)
        value = value + yf[seen(across, "y", unit)].astype(F32)
        value = value + zf[0, seen(last, "zp", unit)].astype(F32)
        value = value + zf[1, seen(last, "zm", unit)].astype(F32)
        for core in range(2):
            at = pl.multiple_of(member(q, k, core) * 64 + h * 32, 32)
            ordered = [value[i * 32 + core * 16:i * 32 + core * 16 + 16] for i in range(2)]
            out[pl.ds(at, 32)] = jnp.concatenate(ordered, axis=0).astype(BF16)

    def have(*units):
        for unit in units:
            for copy in sib[unit]:
                arrived(copy)

    def all_sent(ref, sem):
        pltpu.make_async_remote_copy(
            src_ref=ref, dst_ref=ref, send_sem=sem, recv_sem=rs.at[0],
            device_id=peer["s"], device_id_type=MESH).wait_send()

    have((0, 0, 0), (0, 0, 1))
    pltpu.make_async_copy(w, w, w_sem).wait()
    dot_in(0, 2)
    arrived(zp0[0])
    zp2[0].start()
    sib[0, 3, 0][0].start()
    arrived(zm0[3])
    zm2[0].start()
    sib[0, 1, 1][1].start()
    arrived(y0[0])
    sib[1, 0, 0][0].start()
    pltpu.make_async_copy(dn, dn, d_sem).wait()
    dot_out(0, 2, 0, 8)
    pairs["A"][0].start()
    arrived(zp0[1])
    zp2[1].start()
    zp0[3].start()
    sib[0, 3, 0][1].start()
    arrived(zm0[2])
    zm2[1].start()
    zm0[0].start()
    sib[0, 1, 1][0].start()
    arrived(y0[1])
    sib[1, 0, 0][1].start()
    for i in range(2):
        zpp[i].start()
        zmp[i].start()
    have((0, 3, 0), (0, 1, 1), (1, 0, 0))
    dot_in(2, 3)
    send_leaf("A", ("y",))
    for i in range(2, 4):
        arrived(y0[i])
        zpp[i].start()
        zmp[i].start()
    exchange((1, 0, 1))
    arrived(zp2[0])
    y2[0].start()
    arrived(zm2[0])
    y2[3].start()
    dot_out(2, 3, 0, 8)
    pairs["B"][0].start()
    send_leaf("A", ("zp", "zm"))
    arrived(zp2[1])
    y2[1].start()
    exchange((0, 2, 0))
    arrived(zm2[1])
    y2[2].start()
    exchange((0, 2, 1))
    send_leaf("B")
    have((1, 0, 1), (0, 2, 0), (0, 2, 1))
    dot_in(5, 3)
    arrived(zp0[2])
    arrived(zp0[3])
    exchange((0, 3, 1))
    arrived(zm0[1])
    arrived(zm0[0])
    exchange((0, 1, 0))
    dot_out(5, 3, 0, 8)
    pairs["C"][0].start()
    for copies, unit in ((zpp, (1, 3, 0)), (zmp, (1, 1, 0))):
        arrived(copies[0])
        arrived(copies[1])
        exchange(unit)
    have((0, 3, 1), (0, 1, 0))
    dot_in(8, 2)
    send_leaf("C")
    for h in range(2):
        arrived(y2[2 * h])
        arrived(y2[2 * h + 1])
        exchange((1, 2, h))
    dot_out(8, 2, 0, 8)
    pairs["D"][0].start()
    have((1, 3, 0), (1, 1, 0))
    dot_in(10, 2)
    send_leaf("D")
    for i in (2, 3):
        for copies, unit in ((zpp, (1, 3, 1)), (zmp, (1, 1, 1))):
            arrived(copies[i])
            sib[unit][i - 2].start()
    dot_out(10, 2, 0, 8)
    pairs["E"][0].start()
    have((1, 2, 0), (1, 2, 1))
    dot_in(12, 2)
    send_leaf("E")
    send_half(0)
    send_across(0)
    have((1, 3, 1), (1, 1, 1))
    dot_in(14, 2)
    dot_out(12, 4, 0, 3)
    pairs["G"][0].start()
    pairs["K"][0].start()
    send_half(1)
    dot_out(12, 4, 3, 8)
    pairs["G"][1].start()
    pairs["K"][1].start()
    send_leaf("G", ("y",))
    send_leaf("K")
    send_across(1)
    send_leaf("G", ("zp", "zm"))
    send_last(0)
    send_last(1)
    send_half(2)
    send_half(3)
    send_last(2)
    send_across(2)
    send_across(3)
    send_last(3)
    send_last(4)
    piece = {u: max(last[link][1][SEEN[link](*u)][0] for link in ("zp", "zm")) for u in UNITS}
    for unit in sorted(UNITS, key=lambda u: piece[u]):
        finish(unit)
    all_sent(x.at[pl.ds(0, 15)], x_sem)
    all_sent(sb, pair_sem)
    all_sent(sd, sd_sem)


N_REMOTE = 28 + 16 + 5 + 9 + 7 * 3 + 8 + 4 + 10
ANY, VMEM = pl.BlockSpec(memory_space=pl.ANY), pl.BlockSpec(memory_space=pltpu.VMEM)


def on_device(tokens, norm_gain, gate_weight, up_weight, down_weight):
    return pl.pallas_call(
        kernel,
        out_shape=pltpu.VMEM((ROWS, COLS), BF16),
        in_specs=[ANY, VMEM, ANY, ANY, ANY],
        out_specs=VMEM,
        scratch_shapes=[
            pltpu.VMEM((16, 2, 2, 16, D), BF16),
            pltpu.VMEM((D, 2 * F), BF16),
            pltpu.VMEM((F, D), BF16),
            pltpu.VMEM((2, 4, 16, D), BF16),
            pltpu.VMEM((ROWS, F), BF16),
            pltpu.VMEM((8, ROWS, COLS), F32),
            pltpu.VMEM((8, ROWS, COLS), BF16),
            pltpu.VMEM((8, ROWS, COLS), BF16),
            pltpu.VMEM((7, ROWS, COLS), BF16),
            pltpu.VMEM((ROWS, COLS), BF16),
            pltpu.VMEM((2, 128, COLS), BF16),
            pltpu.VMEM((2, ROWS, COLS), BF16),
            pltpu.VMEM((2, ROWS, 128), BF16),
            pltpu.VMEM((ROWS, COLS), BF16),
            pltpu.VMEM((2, ROWS, COLS), BF16),
            pltpu.SemaphoreType.DMA,
            pltpu.SemaphoreType.DMA,
            pltpu.SemaphoreType.DMA,
            pltpu.SemaphoreType.DMA,
            pltpu.SemaphoreType.DMA,
            pltpu.SemaphoreType.DMA,
            pltpu.SemaphoreType.DMA((N_REMOTE,)),
        ],
        compiler_params=pltpu.CompilerParams(
            collective_id=0, has_side_effects=True, vmem_limit_bytes=62 * 2**20),
    )(tokens.reshape(4, 16, D), norm_gain.reshape(1, D), gate_weight, up_weight, down_weight)


def solution(mesh):
    return jax.shard_map(
        on_device,
        mesh=mesh,
        in_specs=(
            P(("dp", "tensor"), None),
            P(),
            P(None, "tensor"),
            P(None, "tensor"),
            P("tensor", None),
        ),
        out_specs=P("dp", "tensor"),
        check_vma=False,
    )
```

```python
import jax
import jax.numpy as jnp
from jax import lax
from jax.experimental import pallas as pl
from jax.experimental.pallas import tpu as pltpu
from jax.sharding import PartitionSpec as P

MESH = pl.DeviceIdType.MESH
F32, BF16 = jnp.float32, jnp.bfloat16
D, F, ROWS, COLS = 4096, 896, 1024, 256

UNITS = [(0, 0, 0), (0, 0, 1),
         (0, 3, 0), (0, 1, 1), (1, 0, 0),
         (1, 0, 1), (0, 2, 0), (0, 2, 1),
         (0, 3, 1), (0, 1, 0),
         (1, 3, 0), (1, 1, 0),
         (1, 2, 0), (1, 2, 1),
         (1, 3, 1), (1, 1, 1)]
UNIT = {b: i for i, b in enumerate(UNITS)}
QUARTERED = [(0, 3, 0), (0, 1, 1), (1, 0, 0), (0, 2, 0), (0, 2, 1),
             (1, 3, 0), (1, 1, 0), (1, 2, 0), (1, 2, 1)]
CHUNKS = {"A": (0, 2), "B": (2, 3), "C": (5, 3), "D": (8, 2), "E": (10, 2), "G": (12, 2), "K": (14, 2)}
ACROSS_Y = "DG"
DESTS = [(1, 2), (1, 1), (1, 3), (0, 2), (1, 0), (0, 1), (0, 3), (0, 0)]
DEST = {b: i for i, b in enumerate(DESTS)}
HALF = [[(0, 0, 0), (0, 0, 1), (1, 0, 0), (1, 0, 1)],
        [(1, 3, 0), (1, 1, 0), (0, 3, 0), (0, 1, 0)],
        [(1, 2, 0), (1, 2, 1), (0, 2, 0), (0, 2, 1)],
        [(1, 3, 1), (1, 1, 1), (0, 3, 1), (0, 1, 1)]]
ACROSS = [[(0, 0, 0), (0, 0, 1), (0, 2, 0), (0, 2, 1)], [(0, 1, 0), (0, 1, 1), (0, 3, 0), (0, 3, 1)],
          [(1, 0, 0), (1, 1, 0), (1, 3, 0), (1, 2, 0)], [(1, 0, 1), (1, 1, 1), (1, 3, 1), (1, 2, 1)]]
LAST = {link: [[(0, p, 0), (0, p, 1)],
               [(1, p, 0)],
               [(0, 0, 0), (1, 0, 0)],
               [(1, p, 1), (1, 2, 0)],
               [(0, m, 0), (0, m, 1), (1, m, 0), (1, m, 1)],
               [(0, 0, 1), (1, 0, 1), (1, 2, 1), (0, 2, 0), (0, 2, 1)]]
        for link, p, m in (("zp", 3, 1), ("zm", 1, 3))}
SEEN = {
    "zp": lambda q, k, h: (q, (k + 1) % 4, h),
    "zm": lambda q, k, h: (q, (k + 3) % 4, h),
    "y": lambda q, k, h: (1 - q, k, h),
}


def kernel(tok_hbm, gain_ref, gate_hbm, up_hbm, down_hbm, out,
           x, w, dn, res, hid, own, sb, rb, sd, yl, yp, zl, zh, yf, zf,
           tok_sem, w_sem, d_sem, x_sem, pair_sem, sd_sem, rs):
    dp, t = lax.axis_index("dp"), lax.axis_index("tensor")
    hi, z, c = t // 8, lax.rem(t // 2, 4), lax.rem(t, 2)

    def member(q, k, core):
        return (hi if q == 0 else 1 - hi) * 8 + lax.rem(z + k, 4) * 2 + core

    peer = {
        "zp": (dp, member(0, 1, c)),
        "zm": (dp, member(0, 3, c)),
        "y": (dp, member(1, 0, c)),
        "s": (dp, member(0, 0, 1 - c)),
    }
    barrier = pltpu.get_barrier_semaphore()
    for link in ("y", "zp", "zm", "s"):
        pl.semaphore_signal(barrier, inc=1, device_id=peer[link], device_id_type=MESH)

    tok_copy = pltpu.make_async_copy(tok_hbm, res.at[c], tok_sem)
    tok_copy.start()
    count = [0]

    def remote(link, source, dst, sem):
        i = count[0]
        count[0] += 1
        return pltpu.make_async_remote_copy(
            src_ref=source, dst_ref=dst, send_sem=sem, recv_sem=rs.at[i],
            device_id=peer[link], device_id_type=MESH)

    def quarter(q, k, i):
        return x.at[UNIT[q, k, i // 2], i % 2, c]

    def gather(link, source, dst):
        return [remote(link, quarter(*source, i), quarter(*dst, i), x_sem) for i in range(4)]

    zp0, zm0, y0 = gather("zp", (0, 0), (0, 3)), gather("zm", (0, 0), (0, 1)), gather("y", (0, 0), (1, 0))
    zp2 = [remote("zp", quarter(0, 3, i), quarter(0, 2, i), x_sem) for i in (0, 1)]
    zm2 = [remote("zm", quarter(0, 1, i), quarter(0, 2, i), x_sem) for i in (3, 2)]
    zpp, zmp, y2 = gather("zp", (1, 0), (1, 3)), gather("zm", (1, 0), (1, 1)), gather("y", (0, 2), (1, 2))
    sib = {}
    for u in UNITS:
        if u in QUARTERED:
            sib[u] = [remote("s", x.at[UNIT[u], i, c], x.at[UNIT[u], i, c], x_sem) for i in range(2)]
        else:
            sib[u] = [remote("s", x.at[UNIT[u], :, c], x.at[UNIT[u], :, c], x_sem)]

    def rows(lo, n):
        return pl.ds(lo * 64, n * 64)

    pairs, leaf = {}, {}
    for name, (lo, n) in CHUNKS.items():
        at = rows(lo, n)
        cuts = ((0, 3), (3, 5)) if name in "GK" else ((0, 8),)
        pairs[name] = [remote("s", sb.at[pl.ds(a, m), at], rb.at[pl.ds(a, m), at], pair_sem) for a, m in cuts]
        leaf[name] = {"y": remote("y", sd.at[DEST[1, 2], at], yl.at[at], sd_sem)}
        for link, side, dest in (("zp", 0, (1, 1)), ("zm", 1, (1, 3))):
            if name in ACROSS_Y:
                leaf[name][link] = remote("y", sd.at[DEST[dest], at], yp.at[ACROSS_Y.index(name), side], sd_sem)
            else:
                leaf[name][link] = remote(link, sd.at[DEST[dest], at], zl.at[side, at], sd_sem)

    def pieces(orders, make):
        copies, where, at = [], {}, 0
        for i, units in enumerate(orders):
            copies.append(make(rows(at, len(units))))
            for unit in units:
                where[unit] = (i, at)
                at += 1
        return copies, where

    half = {}
    for link, side in (("zp", 0), ("zm", 1)):
        half[link] = pieces(HALF, lambda at: remote(
            link, sd.at[DEST[0, 2], at, pl.ds(side * 128, 128)], zh.at[side, at], sd_sem))
    across = {"y": pieces(ACROSS, lambda at: remote("y", sd.at[DEST[1, 0], at], yf.at[at], sd_sem))}
    last = {}
    for link, side, k in (("zp", 0, 1), ("zm", 1, 3)):
        last[link] = pieces(LAST[link], lambda at: remote(link, sd.at[DEST[0, k], at], zf.at[side, at], sd_sem))

    waited = set()

    def arrived(copy):
        if id(copy) not in waited:
            waited.add(id(copy))
            copy.wait_recv()

    def on_y(unit):
        return [name for name in ACROSS_Y if CHUNKS[name][0] <= UNIT[unit] < sum(CHUNKS[name])]

    def seen_leaf(link, unit):
        at = UNIT[SEEN[link](*unit)]
        for name, (lo, n) in CHUNKS.items():
            if lo <= at < lo + n:
                arrived(leaf[name][link])
        return rows(at, 1)

    def seen(messages, link, unit):
        copies, where = messages[link]
        i, at = where[SEEN[link](*unit)]
        arrived(copies[i])
        return rows(at, 1)

    def exchange(*units):
        for unit in units:
            for copy in sib[unit]:
                copy.start()

    res[1 - c] = jnp.zeros((4, 16, D), BF16)
    tok_copy.wait()
    for j in range(7):
        for part, source in enumerate((gate_hbm, up_hbm)):
            pltpu.make_async_copy(
                source.at[:, pl.ds(j * 128, 128)], w.at[:, pl.ds(j * 256 + part * 128, 128)], w_sem).start()
    gain = gain_ref[...]
    for i in range(4):
        wide = res[c, i].astype(F32)
        square_mean = jnp.mean(wide * wide, axis=1, keepdims=True)
        normed = wide * gain / jnp.sqrt(square_mean + 1e-05)
        x[i // 2, i % 2, c] = normed.astype(BF16)
    pl.semaphore_wait(barrier, 4)

    exchange((0, 0, 0), (0, 0, 1))
    for i in range(2):
        zp0[i].start()
        zm0[3 - i].start()
        y0[i].start()
    y0[2].start()
    y0[3].start()
    def dot_in(lo, n):
        both = jnp.dot(x[pl.ds(lo, n)].reshape(n * 64, D), w[...], preferred_element_type=F32)
        for j in range(7):
            gate, up = both[:, j * 256:j * 256 + 128], both[:, j * 256 + 128:j * 256 + 256]
            hid[rows(lo, n), pl.ds(j * 128, 128)] = (gate / (1.0 + jnp.exp(-gate)) * up).astype(BF16)

    def dot_out(lo, n, first, end):
        part = jnp.dot(hid[rows(lo, n)], dn[:, pl.ds(first * 512, (end - first) * 512)], preferred_element_type=F32)
        for r in range(first, end):
            for side in range(2):
                at = (r - first) * 512 + side * 256
                value = part[:, at:at + 256]
                if lo == 0:
                    core = (1 - c, c)[side]
                    col = pl.multiple_of(member(*DESTS[r], core) * COLS, COLS)
                    add = [res[kk, i, :, pl.ds(col, COLS)].astype(F32) for i in range(4) for kk in range(2)]
                    value = value + jnp.concatenate(add, axis=0)
                if side == 0:
                    sb[r, rows(lo, n)] = value.astype(BF16)
                else:
                    own[r, rows(lo, n)] = value

    def chip_sum(r, unit, rest=True):
        at = UNIT[unit]
        for name, (lo, n) in CHUNKS.items():
            if lo <= at < lo + n:
                arrived(pairs[name][-1 if rest else 0])
        return own[r, rows(at, 1)] + rb[r, rows(at, 1)].astype(F32)

    def send_leaf(name, links=("y", "zp", "zm")):
        lo, n = CHUNKS[name]
        for link in links:
            r = DEST[{"y": (1, 2), "zp": (1, 1), "zm": (1, 3)}[link]]
            for unit in range(lo, lo + n):
                sd[r, rows(unit, 1)] = chip_sum(r, UNITS[unit], False).astype(BF16)
            leaf[name][link].start()

    def send_half(i):
        r = DEST[0, 2]
        where = half["zp"][1]
        for unit in HALF[i]:
            got = seen_leaf("y", unit)
            sd[r, rows(where[unit][1], 1)] = (chip_sum(r, unit) + yl[got].astype(F32)).astype(BF16)
        half["zp"][0][i].start()
        half["zm"][0][i].start()

    def send_across(i):
        r = DEST[1, 0]
        copies, where = across["y"]
        for unit in ACROSS[i]:
            value = chip_sum(r, unit)
            for link, side in (("zp", 0), ("zm", 1)):
                if not on_y(SEEN[link](*unit)):
                    value = value + zl[side, seen_leaf(link, unit)].astype(F32)
            sd[r, rows(where[unit][1], 1)] = value.astype(BF16)
        copies[i].start()

    def send_last(i):
        for link, side, k in (("zp", 0, 1), ("zm", 1, 3)):
            r = DEST[0, k]
            copies, where = last[link]
            for unit in LAST[link][i]:
                value = chip_sum(r, unit)
                theirs = SEEN["y"](*unit)
                for name in on_y(theirs):
                    arrived(leaf[name][link])
                    part = yp[ACROSS_Y.index(name), side, rows(UNIT[theirs] - CHUNKS[name][0], 1)]
                    value = value + part.astype(F32)
                got = zh[side, seen(half, link, unit)].astype(F32)
                keep = (1 - side) * 128
                at = rows(where[unit][1], 1)
                sd[r, at, pl.ds(side * 128, 128)] = (value[:, side * 128:side * 128 + 128] + got).astype(BF16)
                sd[r, at, pl.ds(keep, 128)] = value[:, keep:keep + 128].astype(BF16)
            copies[i].start()

    def finish(unit):
        q, k, h = unit
        value = chip_sum(DEST[0, 0], unit)
        value = value + yf[seen(across, "y", unit)].astype(F32)
        value = value + zf[0, seen(last, "zp", unit)].astype(F32)
        value = value + zf[1, seen(last, "zm", unit)].astype(F32)
        for core in range(2):
            at = pl.multiple_of(member(q, k, core) * 64 + h * 32, 32)
            ordered = [value[i * 32 + core * 16:i * 32 + core * 16 + 16] for i in range(2)]
            out[pl.ds(at, 32)] = jnp.concatenate(ordered, axis=0).astype(BF16)

    def have(*units):
        for unit in units:
            for copy in sib[unit]:
                arrived(copy)

    def all_sent(ref, sem):
        pltpu.make_async_remote_copy(
            src_ref=ref, dst_ref=ref, send_sem=sem, recv_sem=rs.at[0],
            device_id=peer["s"], device_id_type=MESH).wait_send()

    have((0, 0, 0), (0, 0, 1))
    pltpu.make_async_copy(w, w, w_sem).wait()
    for r, (q, k) in enumerate(DESTS):
        for part, core in enumerate((1 - c, c)):
            col = pl.multiple_of(member(q, k, core) * COLS, COLS)
            pltpu.make_async_copy(
                down_hbm.at[:, pl.ds(col, COLS)], dn.at[:, pl.ds((2 * r + part) * COLS, COLS)], d_sem).start()
    dot_in(0, 2)
    arrived(zp0[0])
    zp2[0].start()
    sib[0, 3, 0][0].start()
    arrived(zm0[3])
    zm2[0].start()
    sib[0, 1, 1][1].start()
    arrived(y0[0])
    sib[1, 0, 0][0].start()
    arrived(zp0[1])
    zp2[1].start()
    zp0[2].start()
    zp0[3].start()
    sib[0, 3, 0][1].start()
    arrived(zm0[2])
    zm2[1].start()
    zm0[1].start()
    zm0[0].start()
    sib[0, 1, 1][0].start()
    arrived(y0[1])
    sib[1, 0, 0][1].start()
    for i in range(2):
        zpp[i].start()
        zmp[i].start()
    pltpu.make_async_copy(dn, dn, d_sem).wait()
    dot_out(0, 2, 0, 8)
    pairs["A"][0].start()
    have((0, 3, 0), (0, 1, 1), (1, 0, 0))
    dot_in(2, 3)
    arrived(zp2[0])
    y2[0].start()
    sib[0, 2, 0][0].start()
    arrived(zm2[0])
    y2[3].start()
    sib[0, 2, 1][1].start()
    dot_out(2, 3, 0, 3)
    arrived(zp2[1])
    y2[1].start()
    sib[0, 2, 0][1].start()
    arrived(zm2[1])
    y2[2].start()
    sib[0, 2, 1][0].start()
    arrived(y0[2])
    arrived(y0[3])
    exchange((1, 0, 1))
    dot_out(2, 3, 3, 8)
    pairs["B"][0].start()
    send_leaf("A")
    have((1, 0, 1), (0, 2, 0), (0, 2, 1))
    dot_in(5, 3)
    send_leaf("B")
    for i in range(2, 4):
        zpp[i].start()
        zmp[i].start()
    dot_out(5, 3, 0, 3)
    arrived(zp0[2])
    arrived(zp0[3])
    exchange((0, 3, 1))
    arrived(zm0[1])
    arrived(zm0[0])
    exchange((0, 1, 0))
    dot_out(5, 3, 3, 8)
    pairs["C"][0].start()
    have((0, 3, 1), (0, 1, 0))
    dot_in(8, 2)
    send_leaf("C")
    for copies, unit in ((zpp, (1, 3, 0)), (zmp, (1, 1, 0))):
        arrived(copies[0])
        sib[unit][0].start()
    dot_out(8, 2, 0, 8)
    for copies, unit in ((zpp, (1, 3, 0)), (zmp, (1, 1, 0))):
        arrived(copies[1])
        sib[unit][1].start()
    pairs["D"][0].start()
    have((1, 3, 0), (1, 1, 0))
    for i in (0, 3, 1, 2):
        arrived(y2[i])
        sib[1, 2, i // 2][i % 2].start()
    dot_in(10, 2)
    send_across(0)
    send_leaf("D")
    dot_out(10, 2, 0, 8)
    pairs["E"][0].start()
    send_half(0)
    have((1, 2, 0), (1, 2, 1))
    dot_in(12, 2)
    for copies, unit in ((zpp, (1, 3, 1)), (zmp, (1, 1, 1))):
        arrived(copies[2])
        arrived(copies[3])
        exchange(unit)
    send_leaf("E")
    dot_out(12, 2, 0, 3)
    pairs["G"][0].start()
    send_last(0)
    dot_out(12, 2, 3, 8)
    pairs["G"][1].start()
    send_leaf("G", ("y",))
    send_across(1)
    have((1, 3, 1), (1, 1, 1))
    dot_in(14, 2)
    send_half(1)
    send_last(1)
    dot_out(14, 2, 0, 3)
    pairs["K"][0].start()
    dot_out(14, 2, 3, 8)
    pairs["K"][1].start()
    send_half(2)
    send_leaf("K")
    send_leaf("G", ("zp", "zm"))
    send_last(2)
    send_last(3)
    send_across(2)
    send_half(3)
    send_last(4)
    send_across(3)
    send_last(5)
    sent = (0, 1, 2, 3, 4, 5)
    piece = {u: max(sent.index(last[link][1][SEEN[link](*u)][0]) for link in ("zp", "zm")) for u in UNITS}
    for unit in sorted(UNITS, key=lambda u: piece[u]):
        finish(unit)
    all_sent(x.at[pl.ds(0, 15)], x_sem)
    all_sent(sb, pair_sem)
    all_sent(sd, sd_sem)


N_REMOTE = 28 + 16 + 9 + 9 + 7 * 3 + 8 + 4 + 12
ANY, VMEM = pl.BlockSpec(memory_space=pl.ANY), pl.BlockSpec(memory_space=pltpu.VMEM)


def on_device(tokens, norm_gain, gate_weight, up_weight, down_weight):
    return pl.pallas_call(
        kernel,
        out_shape=pltpu.VMEM((ROWS, COLS), BF16),
        in_specs=[ANY, VMEM, ANY, ANY, ANY],
        out_specs=VMEM,
        scratch_shapes=[
            pltpu.VMEM((16, 2, 2, 16, D), BF16),
            pltpu.VMEM((D, 2 * F), BF16),
            pltpu.VMEM((F, D), BF16),
            pltpu.VMEM((2, 4, 16, D), BF16),
            pltpu.VMEM((ROWS, F), BF16),
            pltpu.VMEM((8, ROWS, COLS), F32),
            pltpu.VMEM((8, ROWS, COLS), BF16),
            pltpu.VMEM((8, ROWS, COLS), BF16),
            pltpu.VMEM((7, ROWS, COLS), BF16),
            pltpu.VMEM((ROWS, COLS), BF16),
            pltpu.VMEM((2, 2, 128, COLS), BF16),
            pltpu.VMEM((2, ROWS, COLS), BF16),
            pltpu.VMEM((2, ROWS, 128), BF16),
            pltpu.VMEM((ROWS, COLS), BF16),
            pltpu.VMEM((2, ROWS, COLS), BF16),
            pltpu.SemaphoreType.DMA,
            pltpu.SemaphoreType.DMA,
            pltpu.SemaphoreType.DMA,
            pltpu.SemaphoreType.DMA,
            pltpu.SemaphoreType.DMA,
            pltpu.SemaphoreType.DMA,
            pltpu.SemaphoreType.DMA((N_REMOTE,)),
        ],
        compiler_params=pltpu.CompilerParams(
            collective_id=0, has_side_effects=True, vmem_limit_bytes=62 * 2**20),
    )(tokens.reshape(4, 16, D), norm_gain.reshape(1, D), gate_weight, up_weight, down_weight)


def solution(mesh):
    return jax.shard_map(
        on_device,
        mesh=mesh,
        in_specs=(
            P(("dp", "tensor"), None),
            P(),
            P(None, "tensor"),
            P(None, "tensor"),
            P("tensor", None),
        ),
        out_specs=P("dp", "tensor"),
        check_vma=False,
    )
```

```python
import jax
import jax.numpy as jnp
from jax import lax
from jax.experimental import pallas as pl
from jax.experimental.pallas import tpu as pltpu
from jax.sharding import PartitionSpec as P

MESH = pl.DeviceIdType.MESH
F32, BF16 = jnp.float32, jnp.bfloat16
D, F, ROWS, COLS = 4096, 896, 1024, 256

UNITS = [(0, 0, 0), (0, 0, 1),
         (0, 3, 0), (0, 1, 1), (1, 0, 0),
         (1, 0, 1), (0, 2, 0), (0, 2, 1),
         (0, 3, 1), (0, 1, 0),
         (1, 3, 0), (1, 1, 0),
         (1, 2, 0), (1, 2, 1),
         (1, 3, 1), (1, 1, 1)]
UNIT = {b: i for i, b in enumerate(UNITS)}
QUARTERED = [(0, 3, 0), (0, 1, 1), (1, 0, 0), (0, 2, 0), (0, 2, 1),
             (1, 3, 0), (1, 1, 0), (1, 2, 0), (1, 2, 1)]
CHUNKS = {"A": (0, 2), "B": (2, 3), "C": (5, 3), "D": (8, 2), "E": (10, 2), "G": (12, 2), "K": (14, 2)}
ACROSS_Y = "DG"
DESTS = [(1, 2), (1, 1), (1, 3), (0, 2), (1, 0), (0, 1), (0, 3), (0, 0)]
DEST = {b: i for i, b in enumerate(DESTS)}
HALF = [[(0, 0, 0), (0, 0, 1), (1, 0, 0), (1, 0, 1)],
        [(1, 3, 0), (1, 1, 0), (0, 3, 0), (0, 1, 0)],
        [(1, 2, 0), (1, 2, 1), (0, 2, 0), (0, 2, 1)],
        [(1, 3, 1), (1, 1, 1), (0, 3, 1), (0, 1, 1)]]
ACROSS = [[(0, 0, 0), (0, 0, 1), (0, 2, 0), (0, 2, 1)], [(0, 1, 0), (0, 1, 1), (0, 3, 0), (0, 3, 1)],
          [(1, 0, 0), (1, 1, 0), (1, 3, 0), (1, 2, 0)], [(1, 0, 1), (1, 1, 1), (1, 3, 1), (1, 2, 1)]]
LAST = {link: [[(0, p, 0), (0, p, 1)],
               [(1, p, 0)],
               [(0, 0, 0), (1, 0, 0)],
               [(1, p, 1), (1, 2, 0)],
               [(0, m, 0), (0, m, 1), (1, m, 0), (1, m, 1)],
               [(0, 0, 1), (1, 0, 1), (1, 2, 1), (0, 2, 0), (0, 2, 1)]]
        for link, p, m in (("zp", 3, 1), ("zm", 1, 3))}
SEEN = {
    "zp": lambda q, k, h: (q, (k + 1) % 4, h),
    "zm": lambda q, k, h: (q, (k + 3) % 4, h),
    "y": lambda q, k, h: (1 - q, k, h),
}


def kernel(tok_hbm, gain_ref, gate_hbm, up_hbm, down_hbm, out,
           x, w, dn, res, hid, own, sb, rb, sd, yl, yp, zl, zh, yf, zf,
           tok_sem, w_sem, d_sem, x_sem, pair_sem, sd_sem, rs):
    dp, t = lax.axis_index("dp"), lax.axis_index("tensor")
    hi, z, c = t // 8, lax.rem(t // 2, 4), lax.rem(t, 2)

    def member(q, k, core):
        return (hi if q == 0 else 1 - hi) * 8 + lax.rem(z + k, 4) * 2 + core

    peer = {
        "zp": (dp, member(0, 1, c)),
        "zm": (dp, member(0, 3, c)),
        "y": (dp, member(1, 0, c)),
        "s": (dp, member(0, 0, 1 - c)),
    }
    barrier = pltpu.get_barrier_semaphore()
    for link in ("y", "zp", "zm", "s"):
        pl.semaphore_signal(barrier, inc=1, device_id=peer[link], device_id_type=MESH)

    tok_copy = pltpu.make_async_copy(tok_hbm, res.at[c], tok_sem)
    tok_copy.start()
    count = [0]

    def remote(link, source, dst, sem):
        i = count[0]
        count[0] += 1
        return pltpu.make_async_remote_copy(
            src_ref=source, dst_ref=dst, send_sem=sem, recv_sem=rs.at[i],
            device_id=peer[link], device_id_type=MESH)

    def quarter(q, k, i):
        return x.at[UNIT[q, k, i // 2], i % 2, c]

    def gather(link, source, dst):
        return [remote(link, quarter(*source, i), quarter(*dst, i), x_sem) for i in range(4)]

    zp0, zm0, y0 = gather("zp", (0, 0), (0, 3)), gather("zm", (0, 0), (0, 1)), gather("y", (0, 0), (1, 0))
    zp2 = [remote("zp", quarter(0, 3, i), quarter(0, 2, i), x_sem) for i in (0, 1)]
    zm2 = [remote("zm", quarter(0, 1, i), quarter(0, 2, i), x_sem) for i in (3, 2)]
    zpp, zmp, y2 = gather("zp", (1, 0), (1, 3)), gather("zm", (1, 0), (1, 1)), gather("y", (0, 2), (1, 2))
    sib = {}
    for u in UNITS:
        if u in QUARTERED:
            sib[u] = [remote("s", x.at[UNIT[u], i, c], x.at[UNIT[u], i, c], x_sem) for i in range(2)]
        else:
            sib[u] = [remote("s", x.at[UNIT[u], :, c], x.at[UNIT[u], :, c], x_sem)]

    def rows(lo, n):
        return pl.ds(lo * 64, n * 64)

    pairs, leaf = {}, {}
    for name, (lo, n) in CHUNKS.items():
        at = rows(lo, n)
        cuts = ((0, 3), (3, 5)) if name in "GK" else ((0, 8),)
        pairs[name] = [remote("s", sb.at[pl.ds(a, m), at], rb.at[pl.ds(a, m), at], pair_sem) for a, m in cuts]
        leaf[name] = {"y": remote("y", sd.at[DEST[1, 2], at], yl.at[at], sd_sem)}
        for link, side, dest in (("zp", 0, (1, 1)), ("zm", 1, (1, 3))):
            if name in ACROSS_Y:
                leaf[name][link] = remote("y", sd.at[DEST[dest], at], yp.at[ACROSS_Y.index(name), side], sd_sem)
            else:
                leaf[name][link] = remote(link, sd.at[DEST[dest], at], zl.at[side, at], sd_sem)

    def pieces(orders, make):
        copies, where, at = [], {}, 0
        for i, units in enumerate(orders):
            copies.append(make(rows(at, len(units))))
            for unit in units:
                where[unit] = (i, at)
                at += 1
        return copies, where

    half = {}
    for link, side in (("zp", 0), ("zm", 1)):
        half[link] = pieces(HALF, lambda at: remote(
            link, sd.at[DEST[0, 2], at, pl.ds(side * 128, 128)], zh.at[side, at], sd_sem))
    across = {"y": pieces(ACROSS, lambda at: remote("y", sd.at[DEST[1, 0], at], yf.at[at], sd_sem))}
    last = {}
    for link, side, k in (("zp", 0, 1), ("zm", 1, 3)):
        last[link] = pieces(LAST[link], lambda at: remote(link, sd.at[DEST[0, k], at], zf.at[side, at], sd_sem))

    waited = set()

    def arrived(copy):
        if id(copy) not in waited:
            waited.add(id(copy))
            copy.wait_recv()

    def on_y(unit):
        return [name for name in ACROSS_Y if CHUNKS[name][0] <= UNIT[unit] < sum(CHUNKS[name])]

    def seen_leaf(link, unit):
        at = UNIT[SEEN[link](*unit)]
        for name, (lo, n) in CHUNKS.items():
            if lo <= at < lo + n:
                arrived(leaf[name][link])
        return rows(at, 1)

    def seen(messages, link, unit):
        copies, where = messages[link]
        i, at = where[SEEN[link](*unit)]
        arrived(copies[i])
        return rows(at, 1)

    def exchange(*units):
        for unit in units:
            for copy in sib[unit]:
                copy.start()

    res[1 - c] = jnp.zeros((4, 16, D), BF16)
    tok_copy.wait()
    for j in range(7):
        for part, source in enumerate((gate_hbm, up_hbm)):
            pltpu.make_async_copy(
                source.at[:, pl.ds(j * 128, 128)], w.at[:, pl.ds(j * 256 + part * 128, 128)], w_sem).start()
    gain = gain_ref[...]
    for i in range(4):
        wide = res[c, i].astype(F32)
        square_mean = jnp.mean(wide * wide, axis=1, keepdims=True)
        normed = wide * gain / jnp.sqrt(square_mean + 1e-05)
        x[i // 2, i % 2, c] = normed.astype(BF16)
    pl.semaphore_wait(barrier, 4)

    exchange((0, 0, 0), (0, 0, 1))
    for i in range(2):
        zp0[i].start()
        zm0[3 - i].start()
        y0[i].start()
    y0[2].start()
    y0[3].start()
    def dot_in(lo, n):
        both = jnp.dot(x[pl.ds(lo, n)].reshape(n * 64, D), w[...], preferred_element_type=F32)
        for j in range(7):
            gate, up = both[:, j * 256:j * 256 + 128], both[:, j * 256 + 128:j * 256 + 256]
            hid[rows(lo, n), pl.ds(j * 128, 128)] = (gate / (1.0 + jnp.exp(-gate)) * up).astype(BF16)

    def dot_out(lo, n, first, end):
        part = jnp.dot(hid[rows(lo, n)], dn[:, pl.ds(first * 512, (end - first) * 512)], preferred_element_type=F32)
        for r in range(first, end):
            for side in range(2):
                at = (r - first) * 512 + side * 256
                value = part[:, at:at + 256]
                if lo == 0:
                    core = (1 - c, c)[side]
                    col = pl.multiple_of(member(*DESTS[r], core) * COLS, COLS)
                    add = [res[kk, i, :, pl.ds(col, COLS)].astype(F32) for i in range(4) for kk in range(2)]
                    value = value + jnp.concatenate(add, axis=0)
                if side == 0:
                    sb[r, rows(lo, n)] = value.astype(BF16)
                else:
                    own[r, rows(lo, n)] = value

    def chip_sum(r, unit, rest=True):
        at = UNIT[unit]
        for name, (lo, n) in CHUNKS.items():
            if lo <= at < lo + n:
                arrived(pairs[name][-1 if rest else 0])
        return own[r, rows(at, 1)] + rb[r, rows(at, 1)].astype(F32)

    def send_leaf(name, links=("y", "zp", "zm")):
        lo, n = CHUNKS[name]
        for link in links:
            r = DEST[{"y": (1, 2), "zp": (1, 1), "zm": (1, 3)}[link]]
            for unit in range(lo, lo + n):
                sd[r, rows(unit, 1)] = chip_sum(r, UNITS[unit], False).astype(BF16)
            leaf[name][link].start()

    def send_half(i):
        r = DEST[0, 2]
        where = half["zp"][1]
        for unit in HALF[i]:
            got = seen_leaf("y", unit)
            sd[r, rows(where[unit][1], 1)] = (chip_sum(r, unit) + yl[got].astype(F32)).astype(BF16)
        half["zp"][0][i].start()
        half["zm"][0][i].start()

    def send_across(i):
        r = DEST[1, 0]
        copies, where = across["y"]
        for unit in ACROSS[i]:
            value = chip_sum(r, unit)
            for link, side in (("zp", 0), ("zm", 1)):
                if not on_y(SEEN[link](*unit)):
                    value = value + zl[side, seen_leaf(link, unit)].astype(F32)
            sd[r, rows(where[unit][1], 1)] = value.astype(BF16)
        copies[i].start()

    def send_last(i):
        for link, side, k in (("zp", 0, 1), ("zm", 1, 3)):
            r = DEST[0, k]
            copies, where = last[link]
            for unit in LAST[link][i]:
                value = chip_sum(r, unit)
                theirs = SEEN["y"](*unit)
                for name in on_y(theirs):
                    arrived(leaf[name][link])
                    part = yp[ACROSS_Y.index(name), side, rows(UNIT[theirs] - CHUNKS[name][0], 1)]
                    value = value + part.astype(F32)
                got = zh[side, seen(half, link, unit)].astype(F32)
                keep = (1 - side) * 128
                at = rows(where[unit][1], 1)
                sd[r, at, pl.ds(side * 128, 128)] = (value[:, side * 128:side * 128 + 128] + got).astype(BF16)
                sd[r, at, pl.ds(keep, 128)] = value[:, keep:keep + 128].astype(BF16)
            copies[i].start()

    def finish(unit):
        q, k, h = unit
        value = chip_sum(DEST[0, 0], unit)
        value = value + yf[seen(across, "y", unit)].astype(F32)
        value = value + zf[0, seen(last, "zp", unit)].astype(F32)
        value = value + zf[1, seen(last, "zm", unit)].astype(F32)
        for core in range(2):
            at = pl.multiple_of(member(q, k, core) * 64 + h * 32, 32)
            ordered = [value[i * 32 + core * 16:i * 32 + core * 16 + 16] for i in range(2)]
            out[pl.ds(at, 32)] = jnp.concatenate(ordered, axis=0).astype(BF16)

    def have(*units):
        for unit in units:
            for copy in sib[unit]:
                arrived(copy)

    def all_sent(ref, sem):
        pltpu.make_async_remote_copy(
            src_ref=ref, dst_ref=ref, send_sem=sem, recv_sem=rs.at[0],
            device_id=peer["s"], device_id_type=MESH).wait_send()

    have((0, 0, 0), (0, 0, 1))
    pltpu.make_async_copy(w, w, w_sem).wait()
    for r, (q, k) in enumerate(DESTS):
        for part, core in enumerate((1 - c, c)):
            col = pl.multiple_of(member(q, k, core) * COLS, COLS)
            pltpu.make_async_copy(
                down_hbm.at[:, pl.ds(col, COLS)], dn.at[:, pl.ds((2 * r + part) * COLS, COLS)], d_sem).start()
    dot_in(0, 2)
    arrived(zp0[0])
    zp2[0].start()
    sib[0, 3, 0][0].start()
    arrived(zm0[3])
    zm2[0].start()
    sib[0, 1, 1][1].start()
    arrived(y0[0])
    sib[1, 0, 0][0].start()
    arrived(zp0[1])
    zp2[1].start()
    zp0[2].start()
    zp0[3].start()
    sib[0, 3, 0][1].start()
    arrived(zm0[2])
    zm2[1].start()
    zm0[1].start()
    zm0[0].start()
    sib[0, 1, 1][0].start()
    arrived(y0[1])
    sib[1, 0, 0][1].start()
    for i in range(2):
        zpp[i].start()
        zmp[i].start()
    pltpu.make_async_copy(dn, dn, d_sem).wait()
    dot_out(0, 2, 0, 8)
    pairs["A"][0].start()
    have((0, 3, 0), (0, 1, 1), (1, 0, 0))
    dot_in(2, 3)
    arrived(zp2[0])
    y2[0].start()
    sib[0, 2, 0][0].start()
    arrived(zm2[0])
    y2[3].start()
    sib[0, 2, 1][1].start()
    dot_out(2, 3, 0, 3)
    arrived(zp2[1])
    y2[1].start()
    sib[0, 2, 0][1].start()
    arrived(zm2[1])
    y2[2].start()
    sib[0, 2, 1][0].start()
    arrived(y0[2])
    arrived(y0[3])
    exchange((1, 0, 1))
    dot_out(2, 3, 3, 8)
    pairs["B"][0].start()
    send_leaf("A")
    have((1, 0, 1), (0, 2, 0), (0, 2, 1))
    dot_in(5, 3)
    send_leaf("B")
    for i in range(2, 4):
        zpp[i].start()
        zmp[i].start()
    dot_out(5, 3, 0, 3)
    arrived(zp0[2])
    arrived(zp0[3])
    exchange((0, 3, 1))
    arrived(zm0[1])
    arrived(zm0[0])
    exchange((0, 1, 0))
    dot_out(5, 3, 3, 8)
    pairs["C"][0].start()
    have((0, 3, 1), (0, 1, 0))
    dot_in(8, 2)
    send_leaf("C")
    for copies, unit in ((zpp, (1, 3, 0)), (zmp, (1, 1, 0))):
        arrived(copies[0])
        sib[unit][0].start()
    dot_out(8, 2, 0, 8)
    for copies, unit in ((zpp, (1, 3, 0)), (zmp, (1, 1, 0))):
        arrived(copies[1])
        sib[unit][1].start()
    pairs["D"][0].start()
    have((1, 3, 0), (1, 1, 0))
    for i in (0, 3, 1, 2):
        arrived(y2[i])
        sib[1, 2, i // 2][i % 2].start()
    send_across(0)
    dot_in(10, 2)
    send_leaf("D")
    dot_out(10, 2, 0, 8)
    pairs["E"][0].start()
    send_half(0)
    have((1, 2, 0), (1, 2, 1))
    dot_in(12, 2)
    for copies, unit in ((zpp, (1, 3, 1)), (zmp, (1, 1, 1))):
        arrived(copies[2])
        arrived(copies[3])
        exchange(unit)
    send_leaf("E")
    dot_out(12, 2, 0, 3)
    pairs["G"][0].start()
    dot_out(12, 2, 3, 8)
    pairs["G"][1].start()
    send_leaf("G", ("y",))
    send_last(0)
    send_across(1)
    have((1, 3, 1), (1, 1, 1))
    dot_in(14, 2)
    send_half(1)
    send_last(1)
    dot_out(14, 2, 0, 3)
    pairs["K"][0].start()
    dot_out(14, 2, 3, 8)
    pairs["K"][1].start()
    send_half(2)
    send_leaf("K")
    send_leaf("G", ("zp", "zm"))
    send_last(2)
    send_last(3)
    send_across(2)
    send_half(3)
    send_last(4)
    send_across(3)
    send_last(5)
    sent = (0, 1, 2, 3, 4, 5)
    piece = {u: max(sent.index(last[link][1][SEEN[link](*u)][0]) for link in ("zp", "zm")) for u in UNITS}
    for unit in sorted(UNITS, key=lambda u: piece[u]):
        finish(unit)
    all_sent(x.at[pl.ds(0, 15)], x_sem)
    all_sent(sb, pair_sem)
    all_sent(sd, sd_sem)


N_REMOTE = 28 + 16 + 9 + 9 + 7 * 3 + 8 + 4 + 12
ANY, VMEM = pl.BlockSpec(memory_space=pl.ANY), pl.BlockSpec(memory_space=pltpu.VMEM)


def on_device(tokens, norm_gain, gate_weight, up_weight, down_weight):
    return pl.pallas_call(
        kernel,
        out_shape=pltpu.VMEM((ROWS, COLS), BF16),
        in_specs=[ANY, VMEM, ANY, ANY, ANY],
        out_specs=VMEM,
        scratch_shapes=[
            pltpu.VMEM((16, 2, 2, 16, D), BF16),
            pltpu.VMEM((D, 2 * F), BF16),
            pltpu.VMEM((F, D), BF16),
            pltpu.VMEM((2, 4, 16, D), BF16),
            pltpu.VMEM((ROWS, F), BF16),
            pltpu.VMEM((8, ROWS, COLS), F32),
            pltpu.VMEM((8, ROWS, COLS), BF16),
            pltpu.VMEM((8, ROWS, COLS), BF16),
            pltpu.VMEM((7, ROWS, COLS), BF16),
            pltpu.VMEM((ROWS, COLS), BF16),
            pltpu.VMEM((2, 2, 128, COLS), BF16),
            pltpu.VMEM((2, ROWS, COLS), BF16),
            pltpu.VMEM((2, ROWS, 128), BF16),
            pltpu.VMEM((ROWS, COLS), BF16),
            pltpu.VMEM((2, ROWS, COLS), BF16),
            pltpu.SemaphoreType.DMA,
            pltpu.SemaphoreType.DMA,
            pltpu.SemaphoreType.DMA,
            pltpu.SemaphoreType.DMA,
            pltpu.SemaphoreType.DMA,
            pltpu.SemaphoreType.DMA,
            pltpu.SemaphoreType.DMA((N_REMOTE,)),
        ],
        compiler_params=pltpu.CompilerParams(
            collective_id=0, has_side_effects=True, vmem_limit_bytes=62 * 2**20),
    )(tokens.reshape(4, 16, D), norm_gain.reshape(1, D), gate_weight, up_weight, down_weight)


def solution(mesh):
    return jax.shard_map(
        on_device,
        mesh=mesh,
        in_specs=(
            P(("dp", "tensor"), None),
            P(),
            P(None, "tensor"),
            P(None, "tensor"),
            P("tensor", None),
        ),
        out_specs=P("dp", "tensor"),
        check_vma=False,
    )
```

```python
import jax
import jax.numpy as jnp
from jax import lax
from jax.experimental import pallas as pl
from jax.experimental.pallas import tpu as pltpu
from jax.sharding import PartitionSpec as P

MESH = pl.DeviceIdType.MESH
F32, BF16 = jnp.float32, jnp.bfloat16
D, F, ROWS, COLS = 4096, 896, 1024, 256

UNITS = [(0, 0, 0), (0, 0, 1),
         (0, 3, 0), (0, 1, 1), (1, 0, 0),
         (1, 0, 1), (0, 2, 0), (0, 2, 1),
         (0, 3, 1), (0, 1, 0),
         (1, 3, 0), (1, 1, 0),
         (1, 2, 0), (1, 2, 1),
         (1, 3, 1), (1, 1, 1)]
UNIT = {b: i for i, b in enumerate(UNITS)}
QUARTERED = [(0, 3, 0), (0, 1, 1), (1, 0, 0), (0, 2, 0), (0, 2, 1),
             (1, 3, 0), (1, 1, 0), (1, 2, 0), (1, 2, 1)]
CHUNKS = {"A": (0, 2), "B": (2, 3), "C": (5, 3), "D": (8, 2), "E": (10, 2), "G": (12, 2), "K": (14, 2)}
ACROSS_Y = "DG"
DESTS = [(1, 2), (1, 1), (1, 3), (0, 2), (1, 0), (0, 1), (0, 3), (0, 0)]
DEST = {b: i for i, b in enumerate(DESTS)}
HALF = [[(0, 0, 0), (0, 0, 1), (1, 0, 0), (1, 0, 1)],
        [(1, 3, 0), (1, 1, 0), (0, 3, 0), (0, 1, 0)],
        [(1, 2, 0), (1, 2, 1), (0, 2, 0), (0, 2, 1)],
        [(1, 3, 1), (1, 1, 1), (0, 3, 1), (0, 1, 1)]]
ACROSS = [[(0, 0, 0), (0, 0, 1), (0, 2, 0), (0, 2, 1)], [(0, 1, 0), (0, 1, 1), (0, 3, 0), (0, 3, 1)],
          [(1, 0, 0), (1, 1, 0), (1, 3, 0), (1, 2, 0)], [(1, 0, 1), (1, 1, 1), (1, 3, 1), (1, 2, 1)]]
LAST = {link: [[(0, p, 0), (0, p, 1)],
               [(1, p, 0)],
               [(0, 0, 0), (1, 0, 0)],
               [(1, p, 1), (1, 2, 0)],
               [(0, m, 0), (0, m, 1), (1, m, 0), (1, m, 1)],
               [(0, 0, 1), (1, 0, 1), (1, 2, 1), (0, 2, 0), (0, 2, 1)]]
        for link, p, m in (("zp", 3, 1), ("zm", 1, 3))}
SEEN = {
    "zp": lambda q, k, h: (q, (k + 1) % 4, h),
    "zm": lambda q, k, h: (q, (k + 3) % 4, h),
    "y": lambda q, k, h: (1 - q, k, h),
}


def kernel(tok_hbm, gain_ref, gate_hbm, up_hbm, down_hbm, out,
           x, w, dn, res, hid, own, sb, rb, sd, yl, yp, zl, zh, yf, zf,
           tok_sem, w_sem, d_sem, x_sem, pair_sem, sd_sem, rs):
    dp, t = lax.axis_index("dp"), lax.axis_index("tensor")
    hi, z, c = t // 8, lax.rem(t // 2, 4), lax.rem(t, 2)

    def member(q, k, core):
        return (hi if q == 0 else 1 - hi) * 8 + lax.rem(z + k, 4) * 2 + core

    peer = {
        "zp": (dp, member(0, 1, c)),
        "zm": (dp, member(0, 3, c)),
        "y": (dp, member(1, 0, c)),
        "s": (dp, member(0, 0, 1 - c)),
    }
    barrier = pltpu.get_barrier_semaphore()
    for link in ("y", "zp", "zm", "s"):
        pl.semaphore_signal(barrier, inc=1, device_id=peer[link], device_id_type=MESH)

    tok_copy = pltpu.make_async_copy(tok_hbm, res.at[c], tok_sem)
    tok_copy.start()
    count = [0]

    def remote(link, source, dst, sem):
        i = count[0]
        count[0] += 1
        return pltpu.make_async_remote_copy(
            src_ref=source, dst_ref=dst, send_sem=sem, recv_sem=rs.at[i],
            device_id=peer[link], device_id_type=MESH)

    def quarter(q, k, i):
        return x.at[UNIT[q, k, i // 2], i % 2, c]

    def gather(link, source, dst):
        return [remote(link, quarter(*source, i), quarter(*dst, i), x_sem) for i in range(4)]

    zp0, zm0, y0 = gather("zp", (0, 0), (0, 3)), gather("zm", (0, 0), (0, 1)), gather("y", (0, 0), (1, 0))
    zp2 = [remote("zp", quarter(0, 3, i), quarter(0, 2, i), x_sem) for i in (0, 1)]
    zm2 = [remote("zm", quarter(0, 1, i), quarter(0, 2, i), x_sem) for i in (3, 2)]
    zpp, zmp, y2 = gather("zp", (1, 0), (1, 3)), gather("zm", (1, 0), (1, 1)), gather("y", (0, 2), (1, 2))
    sib = {}
    for u in UNITS:
        if u in QUARTERED:
            sib[u] = [remote("s", x.at[UNIT[u], i, c], x.at[UNIT[u], i, c], x_sem) for i in range(2)]
        else:
            sib[u] = [remote("s", x.at[UNIT[u], :, c], x.at[UNIT[u], :, c], x_sem)]

    def rows(lo, n):
        return pl.ds(lo * 64, n * 64)

    pairs, leaf = {}, {}
    for name, (lo, n) in CHUNKS.items():
        at = rows(lo, n)
        cuts = ((0, 3), (3, 5)) if name in "GK" else ((0, 8),)
        pairs[name] = [remote("s", sb.at[pl.ds(a, m), at], rb.at[pl.ds(a, m), at], pair_sem) for a, m in cuts]
        leaf[name] = {"y": remote("y", sd.at[DEST[1, 2], at], yl.at[at], sd_sem)}
        for link, side, dest in (("zp", 0, (1, 1)), ("zm", 1, (1, 3))):
            if name in ACROSS_Y:
                leaf[name][link] = remote("y", sd.at[DEST[dest], at], yp.at[ACROSS_Y.index(name), side], sd_sem)
            else:
                leaf[name][link] = remote(link, sd.at[DEST[dest], at], zl.at[side, at], sd_sem)

    def pieces(orders, make):
        copies, where, at = [], {}, 0
        for i, units in enumerate(orders):
            copies.append(make(rows(at, len(units))))
            for unit in units:
                where[unit] = (i, at)
                at += 1
        return copies, where

    half = {}
    for link, side in (("zp", 0), ("zm", 1)):
        half[link] = pieces(HALF, lambda at: remote(
            link, sd.at[DEST[0, 2], at, pl.ds(side * 128, 128)], zh.at[side, at], sd_sem))
    across = {"y": pieces(ACROSS, lambda at: remote("y", sd.at[DEST[1, 0], at], yf.at[at], sd_sem))}
    last = {}
    for link, side, k in (("zp", 0, 1), ("zm", 1, 3)):
        last[link] = pieces(LAST[link], lambda at: remote(link, sd.at[DEST[0, k], at], zf.at[side, at], sd_sem))

    waited = set()

    def arrived(copy):
        if id(copy) not in waited:
            waited.add(id(copy))
            copy.wait_recv()

    def on_y(unit):
        return [name for name in ACROSS_Y if CHUNKS[name][0] <= UNIT[unit] < sum(CHUNKS[name])]

    def seen_leaf(link, unit):
        at = UNIT[SEEN[link](*unit)]
        for name, (lo, n) in CHUNKS.items():
            if lo <= at < lo + n:
                arrived(leaf[name][link])
        return rows(at, 1)

    def seen(messages, link, unit):
        copies, where = messages[link]
        i, at = where[SEEN[link](*unit)]
        arrived(copies[i])
        return rows(at, 1)

    def exchange(*units):
        for unit in units:
            for copy in sib[unit]:
                copy.start()

    res[1 - c] = jnp.zeros((4, 16, D), BF16)
    tok_copy.wait()
    for j in range(7):
        for part, source in enumerate((gate_hbm, up_hbm)):
            pltpu.make_async_copy(
                source.at[:, pl.ds(j * 128, 128)], w.at[:, pl.ds(j * 256 + part * 128, 128)], w_sem).start()
    gain = gain_ref[...]
    for i in range(4):
        wide = res[c, i].astype(F32)
        square_mean = jnp.mean(wide * wide, axis=1, keepdims=True)
        normed = wide * gain / jnp.sqrt(square_mean + 1e-05)
        x[i // 2, i % 2, c] = normed.astype(BF16)
    pl.semaphore_wait(barrier, 4)

    exchange((0, 0, 0), (0, 0, 1))
    for i in range(2):
        zp0[i].start()
        zm0[3 - i].start()
        y0[i].start()
    y0[2].start()
    y0[3].start()
    def dot_in(lo, n):
        both = jnp.dot(x[pl.ds(lo, n)].reshape(n * 64, D), w[...], preferred_element_type=F32)
        for j in range(7):
            gate, up = both[:, j * 256:j * 256 + 128], both[:, j * 256 + 128:j * 256 + 256]
            hid[rows(lo, n), pl.ds(j * 128, 128)] = (gate / (1.0 + jnp.exp(-gate)) * up).astype(BF16)

    def dot_out(lo, n, first, end):
        part = jnp.dot(hid[rows(lo, n)], dn[:, pl.ds(first * 512, (end - first) * 512)], preferred_element_type=F32)
        for r in range(first, end):
            for side in range(2):
                at = (r - first) * 512 + side * 256
                value = part[:, at:at + 256]
                if lo == 0:
                    core = (1 - c, c)[side]
                    col = pl.multiple_of(member(*DESTS[r], core) * COLS, COLS)
                    add = [res[kk, i, :, pl.ds(col, COLS)].astype(F32) for i in range(4) for kk in range(2)]
                    value = value + jnp.concatenate(add, axis=0)
                if side == 0:
                    sb[r, rows(lo, n)] = value.astype(BF16)
                else:
                    own[r, rows(lo, n)] = value

    def chip_sum(r, unit, rest=True):
        at = UNIT[unit]
        for name, (lo, n) in CHUNKS.items():
            if lo <= at < lo + n:
                arrived(pairs[name][-1 if rest else 0])
        return own[r, rows(at, 1)] + rb[r, rows(at, 1)].astype(F32)

    def send_leaf(name, links=("y", "zp", "zm")):
        lo, n = CHUNKS[name]
        for link in links:
            r = DEST[{"y": (1, 2), "zp": (1, 1), "zm": (1, 3)}[link]]
            for unit in range(lo, lo + n):
                sd[r, rows(unit, 1)] = chip_sum(r, UNITS[unit], False).astype(BF16)
            leaf[name][link].start()

    def send_half(i):
        r = DEST[0, 2]
        where = half["zp"][1]
        for unit in HALF[i]:
            got = seen_leaf("y", unit)
            sd[r, rows(where[unit][1], 1)] = (chip_sum(r, unit) + yl[got].astype(F32)).astype(BF16)
        half["zp"][0][i].start()
        half["zm"][0][i].start()

    def send_across(i):
        r = DEST[1, 0]
        copies, where = across["y"]
        for unit in ACROSS[i]:
            value = chip_sum(r, unit)
            for link, side in (("zp", 0), ("zm", 1)):
                if not on_y(SEEN[link](*unit)):
                    value = value + zl[side, seen_leaf(link, unit)].astype(F32)
            sd[r, rows(where[unit][1], 1)] = value.astype(BF16)
        copies[i].start()

    def send_last(i):
        for link, side, k in (("zp", 0, 1), ("zm", 1, 3)):
            r = DEST[0, k]
            copies, where = last[link]
            for unit in LAST[link][i]:
                value = chip_sum(r, unit)
                theirs = SEEN["y"](*unit)
                for name in on_y(theirs):
                    arrived(leaf[name][link])
                    part = yp[ACROSS_Y.index(name), side, rows(UNIT[theirs] - CHUNKS[name][0], 1)]
                    value = value + part.astype(F32)
                got = zh[side, seen(half, link, unit)].astype(F32)
                keep = (1 - side) * 128
                at = rows(where[unit][1], 1)
                sd[r, at, pl.ds(side * 128, 128)] = (value[:, side * 128:side * 128 + 128] + got).astype(BF16)
                sd[r, at, pl.ds(keep, 128)] = value[:, keep:keep + 128].astype(BF16)
            copies[i].start()

    def finish(unit):
        q, k, h = unit
        value = chip_sum(DEST[0, 0], unit)
        value = value + yf[seen(across, "y", unit)].astype(F32)
        value = value + zf[0, seen(last, "zp", unit)].astype(F32)
        value = value + zf[1, seen(last, "zm", unit)].astype(F32)
        for core in range(2):
            at = pl.multiple_of(member(q, k, core) * 64 + h * 32, 32)
            ordered = [value[i * 32 + core * 16:i * 32 + core * 16 + 16] for i in range(2)]
            out[pl.ds(at, 32)] = jnp.concatenate(ordered, axis=0).astype(BF16)

    def have(*units):
        for unit in units:
            for copy in sib[unit]:
                arrived(copy)

    def all_sent(ref, sem):
        pltpu.make_async_remote_copy(
            src_ref=ref, dst_ref=ref, send_sem=sem, recv_sem=rs.at[0],
            device_id=peer["s"], device_id_type=MESH).wait_send()

    have((0, 0, 0), (0, 0, 1))
    pltpu.make_async_copy(w, w, w_sem).wait()
    for r, (q, k) in enumerate(DESTS):
        for part, core in enumerate((1 - c, c)):
            col = pl.multiple_of(member(q, k, core) * COLS, COLS)
            pltpu.make_async_copy(
                down_hbm.at[:, pl.ds(col, COLS)], dn.at[:, pl.ds((2 * r + part) * COLS, COLS)], d_sem).start()
    arrived(zp0[0])
    zp2[0].start()
    sib[0, 3, 0][0].start()
    arrived(zm0[3])
    zm2[0].start()
    sib[0, 1, 1][1].start()
    arrived(y0[0])
    sib[1, 0, 0][0].start()
    dot_in(0, 2)
    arrived(zp0[1])
    zp2[1].start()
    zp0[2].start()
    zp0[3].start()
    sib[0, 3, 0][1].start()
    arrived(zm0[2])
    zm2[1].start()
    zm0[1].start()
    zm0[0].start()
    sib[0, 1, 1][0].start()
    arrived(y0[1])
    sib[1, 0, 0][1].start()
    for i in range(2):
        zpp[i].start()
        zmp[i].start()
    pltpu.make_async_copy(dn, dn, d_sem).wait()
    dot_out(0, 2, 0, 8)
    pairs["A"][0].start()
    have((0, 3, 0), (0, 1, 1), (1, 0, 0))
    dot_in(2, 3)
    arrived(zp2[0])
    y2[0].start()
    sib[0, 2, 0][0].start()
    arrived(zm2[0])
    y2[3].start()
    sib[0, 2, 1][1].start()
    dot_out(2, 3, 0, 3)
    arrived(zp2[1])
    y2[1].start()
    sib[0, 2, 0][1].start()
    arrived(zm2[1])
    y2[2].start()
    sib[0, 2, 1][0].start()
    arrived(y0[2])
    arrived(y0[3])
    exchange((1, 0, 1))
    dot_out(2, 3, 3, 8)
    pairs["B"][0].start()
    send_leaf("A")
    have((1, 0, 1), (0, 2, 0), (0, 2, 1))
    dot_in(5, 3)
    send_leaf("B")
    for i in range(2, 4):
        zpp[i].start()
        zmp[i].start()
    dot_out(5, 3, 0, 3)
    arrived(zp0[2])
    arrived(zp0[3])
    exchange((0, 3, 1))
    arrived(zm0[1])
    arrived(zm0[0])
    exchange((0, 1, 0))
    dot_out(5, 3, 3, 8)
    pairs["C"][0].start()
    have((0, 3, 1), (0, 1, 0))
    dot_in(8, 2)
    send_leaf("C")
    for copies, unit in ((zpp, (1, 3, 0)), (zmp, (1, 1, 0))):
        arrived(copies[0])
        sib[unit][0].start()
    dot_out(8, 2, 0, 8)
    for copies, unit in ((zpp, (1, 3, 0)), (zmp, (1, 1, 0))):
        arrived(copies[1])
        sib[unit][1].start()
    pairs["D"][0].start()
    have((1, 3, 0), (1, 1, 0))
    for i in (0, 3, 1, 2):
        arrived(y2[i])
        sib[1, 2, i // 2][i % 2].start()
    send_across(0)
    dot_in(10, 2)
    send_leaf("D")
    dot_out(10, 2, 0, 8)
    pairs["E"][0].start()
    send_half(0)
    have((1, 2, 0), (1, 2, 1))
    dot_in(12, 2)
    for copies, unit in ((zpp, (1, 3, 1)), (zmp, (1, 1, 1))):
        arrived(copies[2])
        arrived(copies[3])
        exchange(unit)
    send_leaf("E")
    dot_out(12, 2, 0, 3)
    pairs["G"][0].start()
    dot_out(12, 2, 3, 8)
    pairs["G"][1].start()
    send_leaf("G", ("y",))
    send_last(0)
    send_across(1)
    have((1, 3, 1), (1, 1, 1))
    dot_in(14, 2)
    send_half(1)
    send_last(1)
    dot_out(14, 2, 0, 3)
    pairs["K"][0].start()
    dot_out(14, 2, 3, 8)
    pairs["K"][1].start()
    send_half(2)
    send_leaf("K")
    send_leaf("G", ("zp", "zm"))
    send_last(2)
    send_last(3)
    send_across(2)
    send_half(3)
    send_last(4)
    send_across(3)
    send_last(5)
    sent = (0, 1, 2, 3, 4, 5)
    piece = {u: max(sent.index(last[link][1][SEEN[link](*u)][0]) for link in ("zp", "zm")) for u in UNITS}
    for unit in sorted(UNITS, key=lambda u: piece[u]):
        finish(unit)
    all_sent(x.at[pl.ds(0, 15)], x_sem)
    all_sent(sb, pair_sem)
    all_sent(sd, sd_sem)


N_REMOTE = 28 + 16 + 9 + 9 + 7 * 3 + 8 + 4 + 12
ANY, VMEM = pl.BlockSpec(memory_space=pl.ANY), pl.BlockSpec(memory_space=pltpu.VMEM)


def on_device(tokens, norm_gain, gate_weight, up_weight, down_weight):
    return pl.pallas_call(
        kernel,
        out_shape=pltpu.VMEM((ROWS, COLS), BF16),
        in_specs=[ANY, VMEM, ANY, ANY, ANY],
        out_specs=VMEM,
        scratch_shapes=[
            pltpu.VMEM((16, 2, 2, 16, D), BF16),
            pltpu.VMEM((D, 2 * F), BF16),
            pltpu.VMEM((F, D), BF16),
            pltpu.VMEM((2, 4, 16, D), BF16),
            pltpu.VMEM((ROWS, F), BF16),
            pltpu.VMEM((8, ROWS, COLS), F32),
            pltpu.VMEM((8, ROWS, COLS), BF16),
            pltpu.VMEM((8, ROWS, COLS), BF16),
            pltpu.VMEM((7, ROWS, COLS), BF16),
            pltpu.VMEM((ROWS, COLS), BF16),
            pltpu.VMEM((2, 2, 128, COLS), BF16),
            pltpu.VMEM((2, ROWS, COLS), BF16),
            pltpu.VMEM((2, ROWS, 128), BF16),
            pltpu.VMEM((ROWS, COLS), BF16),
            pltpu.VMEM((2, ROWS, COLS), BF16),
            pltpu.SemaphoreType.DMA,
            pltpu.SemaphoreType.DMA,
            pltpu.SemaphoreType.DMA,
            pltpu.SemaphoreType.DMA,
            pltpu.SemaphoreType.DMA,
            pltpu.SemaphoreType.DMA,
            pltpu.SemaphoreType.DMA((N_REMOTE,)),
        ],
        compiler_params=pltpu.CompilerParams(
            collective_id=0, has_side_effects=True, vmem_limit_bytes=62 * 2**20),
    )(tokens.reshape(4, 16, D), norm_gain.reshape(1, D), gate_weight, up_weight, down_weight)


def solution(mesh):
    return jax.shard_map(
        on_device,
        mesh=mesh,
        in_specs=(
            P(("dp", "tensor"), None),
            P(),
            P(None, "tensor"),
            P(None, "tensor"),
            P("tensor", None),
        ),
        out_specs=P("dp", "tensor"),
        check_vma=False,
    )
```
